32 devices in a mesh: gx: 2 (over x), gy: 4 (over z), gz: 4 (over y, core).
Axes of the slice: x: 2, y: 2, z: 4, core: 2. Of those that a mesh axis runs over, the one named last changes fastest.
Arguments:
- pair_map: bfloat16 [160, 160, 128], P('gx', ('gy', 'gz')), may hold values from -6 to 6
- residue_mask: int32 [160], replicated, may hold values 0 or 1
- proj_weight: bfloat16 [128, 512], replicated, may hold values from -0.5 to 0.5
- gate_weight: bfloat16 [128, 128], replicated, may hold values from -0.5 to 0.5
- out_weight: bfloat16 [128, 128], replicated, may hold values from -0.5 to 0.5
Outputs:
- update: bfloat16 [160, 160, 128], P('gx', ('gy', 'gz'))
The draws below stay inside these ranges and needn't reach their ends.
All inputs are finite; a program needn't handle non-finite values.
Results may differ from the reference program's by a relative error of at most 0.009.
Values may be sent and summed in bfloat16 or wider, within the bound.
A program may use at most 128 MiB of HBM per device.

```python
import jax
import jax.numpy as jnp
from jax import lax

C = 128
HID = 128
RES_DEV = 80
N = 160


def touch_ends(result, key, least, top_value):
    dims = result.shape
    place = [jax.random.randint(jax.random.fold_in(key, axis), (), 0, dims[axis]) for axis in range(len(dims))]
    result = result.at[tuple(place)].set(least)
    longest = dims.index(max(dims))
    place[longest] = (place[longest] + 1) % dims[longest]
    return result.at[tuple(place)].set(top_value)


def steps_of(own_key, dims, pieces, smallest, high):
    gain, own = 1.0, jax.random.fold_in(own_key, 6)
    for axis_at, parts in pieces:
        heights = jnp.exp(jax.random.uniform(jax.random.fold_in(own, axis_at), (parts,), jnp.float32, smallest / len(pieces), high / len(pieces)))
        gain = gain * jnp.repeat(heights, dims[axis_at] // parts).reshape([-1 if axis == axis_at else 1 for axis in range(len(dims))])
    return gain


def gaussian(own_key, extent, deviation, bound, pieces=(), kind=jnp.bfloat16):
    entries = deviation * jax.random.normal(own_key, extent, jnp.float32)
    if pieces:
        entries = entries * steps_of(own_key, extent, pieces, -0.22, 0.18)
    return jnp.clip(entries, -bound, bound).astype(kind)


def setup_inputs(seed: int = 0) -> dict:
    splits = jax.random.split(jax.random.key(seed), 6)
    pair_map = gaussian(splits[0], (N, N, C), 1.0, 6.0, ((0, 2), (1, 16)))
    residue_mask = touch_ends((jax.random.randint(splits[1], (N,), 0, 8) < 7).astype(jnp.int32), jax.random.fold_in(splits[1], 1), 0, 1)
    proj_weight = gaussian(splits[2], (C, 4 * HID), C ** -0.5, 0.5)
    gate_weight = gaussian(splits[3], (C, C), C ** -0.5, 0.5)
    out_weight = gaussian(splits[4], (HID, C), HID ** -0.5, 0.5)
    return {"pair_map": pair_map, "residue_mask": residue_mask, "proj_weight": proj_weight, "gate_weight": gate_weight, "out_weight": out_weight}


epsilon = 1.0

def layer_norm(values):
    average = lax.optimization_barrier(jnp.mean(values, axis=-1, keepdims=True))
    centred = values - average
    variance = lax.optimization_barrier(jnp.mean(centred * centred, axis=-1, keepdims=True))
    return centred * lax.rsqrt(variance + epsilon)

def reference(pair_map, residue_mask, proj_weight, gate_weight, out_weight):
    mask_float = residue_mask.astype(jnp.float32)

    def project(inputs):
        row_block, row_mask = inputs
        normed = layer_norm(row_block.astype(jnp.float32)).astype(jnp.bfloat16)
        flattened = normed.reshape(-1, C)
        projected = jnp.dot(flattened, proj_weight, preferred_element_type=jnp.float32).reshape(RES_DEV, N, 4 * HID)
        pair_mask = (row_mask[:, None] * mask_float[None, :])[:, :, None]
        left_proj = (jax.nn.sigmoid(projected[:, :, :HID]) * projected[:, :, HID:2 * HID] * pair_mask).astype(jnp.bfloat16)
        right_proj = (jax.nn.sigmoid(projected[:, :, 2 * HID:3 * HID]) * projected[:, :, 3 * HID:] * pair_mask).astype(jnp.bfloat16)
        gate_value = jax.nn.sigmoid(jnp.dot(flattened, gate_weight, preferred_element_type=jnp.float32)).reshape(RES_DEV, N, C)
        return (left_proj, right_proj, gate_value)
    blocks = pair_map.reshape(N // RES_DEV, RES_DEV, N, C)
    mask_blocks = mask_float.reshape(N // RES_DEV, RES_DEV)
    left_proj, right_proj, gate_value = lax.map(project, (blocks, mask_blocks))
    right_wide = right_proj.reshape(N, N, HID).astype(jnp.float32)

    def finish(inputs):
        left_block, gate_block = inputs
        triangle = jnp.einsum('ikc,jkc->ijc', left_block.astype(jnp.float32), right_wide).astype(jnp.bfloat16)
        normed_tri = layer_norm(triangle.astype(jnp.float32)).astype(jnp.bfloat16)
        mixed_out = jnp.dot(normed_tri.reshape(-1, HID), out_weight, preferred_element_type=jnp.float32).reshape(RES_DEV, N, C)
        return (gate_block * mixed_out).astype(jnp.bfloat16)
    update = lax.map(finish, (left_proj, gate_value))
    return update.reshape(N, N, C)
```

```python
import functools

import jax
import jax.numpy as jnp
from jax import lax
from jax.experimental import pallas as pl
from jax.experimental.pallas import tpu as pltpu
from jax.sharding import PartitionSpec as P

epsilon = 1.0


def partner_2(x, axis, bit):
    return lax.ppermute(x, axis, [(i, i ^ 1 << bit) for i in range(lax.axis_size(axis))])


def layer_norm_lead(values):
    average = jnp.mean(values, axis=0, keepdims=True)
    centred = values - average
    variance = jnp.mean(centred * centred, axis=0, keepdims=True)
    return centred * lax.rsqrt(variance + epsilon)


def layer_norm_last(values):
    average = jnp.mean(values, axis=-1, keepdims=True)
    centred = values - average
    variance = jnp.mean(centred * centred, axis=-1, keepdims=True)
    return centred * lax.rsqrt(variance + epsilon)


def swap_with(values, bit):
    return partner_2(values, "gx", bit)


def pair_join(values, bit, position):
    partner = swap_with(values, bit)
    mine_first = position // 2**bit % 2 == 0
    return jnp.where(
        mine_first,
        jnp.concatenate([values, partner], axis=1),
        jnp.concatenate([partner, values], axis=1),
    )


def whole_channels(gathered, out_weight, gate_value):
    hidden, row_count, col_count = gathered.shape
    normed_tri = layer_norm_lead(gathered.astype(jnp.float32)).astype(jnp.bfloat16)
    mixed_out = lax.dot_general(
        normed_tri.reshape(hidden, row_count * col_count),
        out_weight,
        (((0,), (0,)), ((), ())),
        preferred_element_type=jnp.float32,
    )
    return gate_value * mixed_out.reshape(row_count, col_count, out_weight.shape[1])


def local(pair_map, residue_mask, proj_weight, gate_weight, out_weight):
    row_count, col_count, chan_count = pair_map.shape
    hidden = out_weight.shape[0]
    residues = residue_mask.shape[0]
    along_x = lax.axis_size("gx")
    along_y = lax.axis_size("gy")
    along_z = lax.axis_size("gz")
    mask_float = residue_mask.astype(jnp.float32)
    row_mask = lax.dynamic_slice_in_dim(mask_float, lax.axis_index("gx") * row_count, row_count)
    col_mask = lax.dynamic_slice_in_dim(
        mask_float, (lax.axis_index("gy") * along_z + lax.axis_index("gz")) * col_count, col_count
    )
    normed = layer_norm_last(pair_map.astype(jnp.float32)).astype(jnp.bfloat16)
    flattened = normed.reshape(row_count * col_count, chan_count)
    projected = lax.dot_general(
        proj_weight, flattened, (((0,), (1,)), ((), ())), preferred_element_type=jnp.float32
    ).reshape(4 * hidden, row_count, col_count)
    pair_mask = (row_mask[:, None] * col_mask[None, :])[None, :, :]
    left_proj = (
        jax.nn.sigmoid(projected[:hidden]) * projected[hidden : 2 * hidden] * pair_mask
    ).astype(jnp.bfloat16)
    right_proj = (
        jax.nn.sigmoid(projected[2 * hidden : 3 * hidden]) * projected[3 * hidden :] * pair_mask
    ).astype(jnp.bfloat16)
    gate_value = jax.nn.sigmoid(
        jnp.dot(flattened, gate_weight, preferred_element_type=jnp.float32)
    ).reshape(row_count, col_count, chan_count)
    group_count = along_y * along_z
    group_chan = hidden // group_count
    left_group, right_group = (
        lax.all_to_all(left_proj, ("gy", "gz"), split_axis=0, concat_axis=2, tiled=True),
        lax.all_to_all(right_proj, ("gy", "gz"), split_axis=0, concat_axis=2, tiled=True),
    )
    levels = along_x.bit_length() - 1
    low_bits = levels // 2
    high_count = 2 ** (levels - low_bits)
    low_count = 2**low_bits
    position = lax.axis_index("gx")
    left_tile = left_group
    for bit in range(low_bits):
        left_tile = pair_join(left_tile, bit, position)
    right_tile = right_group
    for bit in range(low_bits, levels):
        right_tile = pair_join(right_tile, bit, position)
    block_tile = jnp.einsum(
        "cik,cjk->cij", left_tile, right_tile, preferred_element_type=jnp.float32
    ).astype(jnp.bfloat16)
    for bit in range(low_bits):
        current = block_tile.shape[1]
        span = block_tile.shape[2]
        shaped = block_tile.reshape(group_chan, current // (2 * row_count), 2, row_count, span)
        own_bit = position // 2**bit % 2
        kept = lax.dynamic_index_in_dim(shaped, own_bit, axis=2, keepdims=False).reshape(
            group_chan, current // 2, span
        )
        sent = lax.dynamic_index_in_dim(shaped, 1 - own_bit, axis=2, keepdims=False).reshape(
            group_chan, current // 2, span
        )
        arrived = swap_with(sent, bit)
        block_tile = jnp.where(
            own_bit == 0,
            jnp.concatenate([kept, arrived], axis=2),
            jnp.concatenate([arrived, kept], axis=2),
        )
    block_tile = (
        block_tile.reshape(group_chan, row_count, low_count, high_count, row_count)
        .transpose(0, 1, 3, 2, 4)
        .reshape(group_chan, row_count, residues)
    )
    gathered = lax.all_to_all(block_tile, ("gy", "gz"), split_axis=2, concat_axis=0, tiled=True)
    update = whole_channels(gathered, out_weight, gate_value)
    return update.astype(jnp.bfloat16)


MESH = pl.DeviceIdType.MESH
LANES = 128
HALF_LANES = 64
VMEM_ALL = 67043328
VMEM_BUDGET = 48 * 2**20


def up(value, step):
    return -(-value // step) * step


def gate_by(gate, value):
    return (0.5 * value) * (1.0 + jnp.tanh(0.5 * gate))


def fused_kernel(
    along_y, along_z, main,
    pair_hbm, mask_hbm, proj_hbm, gate_hbm, out_w_hbm, out_ref,
    pair_ref, mask_ref, proj_ref, gate_ref, out_w_ref,
    proj_s, normed_bf, masked_bf, gate_f32, send_r, recv_r, recv_x, send_l, recv_l,
    left_s, edge_s, right_s, right_bf, tri_s, send_e, recv_e, send_b, recv_b,
    load_sem, send_sem, rsem_r, rsem_x, rsem_l, rsem_b,
):
    cols, rows, chans = pair_ref.shape
    hidden = out_w_ref.shape[0]
    groups = along_y * along_z
    gc = hidden // groups
    edge = rows - main
    flat_m, flat_e = main * cols, edge * cols
    flat = flat_m + flat_e
    wide = up(flat, LANES)
    residues = mask_ref.shape[1]
    px, py, pz = lax.axis_index("gx"), lax.axis_index("gy"), lax.axis_index("gz")
    me = py * along_z + pz
    side = py // (along_y // 2)
    middle = along_y // 2

    def place(d):
        return (px, d // along_z, d % along_z)

    far_a, far_b = (1 - side) * middle, (1 - side) * middle + 1
    sibling = side * middle + (py + 1) % middle

    def to(plane, n):
        return plane * along_z + (pz + n) % along_z

    def source(plane, n):
        return plane * along_z + (pz + along_z - n) % along_z

    def turn_of(s):
        return (pz + along_z - s % along_z) % along_z

    partner = (1 - px, py, pz)
    barrier = pltpu.get_barrier_semaphore()

    def greet(o, carry):
        pl.semaphore_signal(barrier, inc=1, device_id=place((me + o) % groups), device_id_type=MESH)
        return carry

    with jax.named_scope("greet"):
        lax.fori_loop(1, groups, greet, 0)
        pl.semaphore_signal(barrier, inc=1, device_id=partner, device_id_type=MESH)

    loads = [
        pltpu.make_async_copy(source, target, load_sem.at[n])
        for n, (source, target) in enumerate(
            (
                (pair_hbm, pair_ref), (mask_hbm, mask_ref), (proj_hbm, proj_ref),
                (gate_hbm, gate_ref), (out_w_hbm, out_w_ref),
            )
        )
    ]
    for load in loads:
        load.start()
    with jax.named_scope("waitload"):
        loads[1].wait()
        loads[2].wait()
        proj_s[...] = proj_ref[...].astype(jnp.float32).T.astype(jnp.bfloat16)
        loads[0].wait()

    with jax.named_scope("norm"):
        mask_f = mask_ref[...].astype(jnp.float32)
        lane = lax.broadcasted_iota(jnp.int32, (rows, residues), 1)
        sub = lax.broadcasted_iota(jnp.int32, (rows, residues), 0)
        row_mask = jnp.sum(jnp.where(lane == sub + px * rows, mask_f, 0.0), axis=1, keepdims=True)
        lane_row = lax.broadcasted_iota(jnp.int32, (1, residues), 1)
        for k in range(cols):
            col_mask = jnp.sum(
                jnp.where(lane_row == me * cols + k, mask_f, 0.0), axis=1, keepdims=True
            )
            normed = layer_norm_last(pair_ref[k].astype(jnp.float32)).astype(jnp.bfloat16)
            masked = (normed.astype(jnp.float32) * (row_mask * col_mask)).astype(jnp.bfloat16)
            for target, value in ((normed_bf, normed), (masked_bf, masked)):
                target[k * main : (k + 1) * main, :] = value[0:main]
                target[flat_m + k * edge : flat_m + (k + 1) * edge, :] = value[main:rows]

    half = hidden // 2
    half_groups = groups // 2

    def gated(base, first, low, high):
        both = jnp.concatenate(
            [
                proj_s[pl.ds(pl.multiple_of(base + first, half), half), :],
                proj_s[pl.ds(pl.multiple_of(base + hidden + first, half), half), :],
            ],
            axis=0,
        )
        both = lax.dot_general(
            both, masked_bf[low:high, :], (((1,), (1,)), ((), ())),
            preferred_element_type=jnp.float32,
        )
        return gate_by(both[0:half], both[half:])

    def copy_r(d, slot):
        return pltpu.make_async_remote_copy(
            src_ref=send_r.at[d], dst_ref=recv_r.at[slot], send_sem=send_sem.at[0],
            recv_sem=rsem_r.at[slot], device_id=place(d), device_id_type=MESH,
        )

    def copy_x(s, count=1):
        return pltpu.make_async_remote_copy(
            src_ref=recv_r.at[pl.ds(s, count), :, 0:wide], dst_ref=recv_x.at[pl.ds(s, count)],
            send_sem=send_sem.at[1], recv_sem=rsem_x.at[turn_of(s)],
            device_id=partner, device_id_type=MESH,
        )

    def copy_many(source, target, kind, recv_sem, d, slot, count=1):
        return pltpu.make_async_remote_copy(
            src_ref=source.at[pl.ds(d, count)], dst_ref=target.at[pl.ds(slot, count)],
            send_sem=send_sem.at[kind], recv_sem=recv_sem, device_id=place(d),
            device_id_type=MESH,
        )

    def copy_l(d, slot, n, count=1):
        return copy_many(send_l, recv_l, 2, rsem_l.at[n], d, slot, count)

    def copy_e(d, slot, count=1):
        return copy_many(send_e, recv_e, 3, rsem_b.at[0], d, slot, count)

    def copy_b(d, slot, count=1):
        return copy_many(send_b, recv_b, 4, rsem_b.at[1], d, slot, count)

    for turn in range(2):
        first = (1 - side if turn == 0 else side) * half
        with jax.named_scope(f"gated_r{turn}"):
            value = gated(2 * hidden, first, 0, flat)
            extra = gated(0, first, flat_m, flat)
            value = jnp.concatenate([value, extra], axis=1)
            for part in range(half_groups):
                send_r[first // gc + part, :, 0 : flat + flat_e] = value[
                    part * gc : (part + 1) * gc
                ].astype(jnp.bfloat16)
        if turn == 0:
            with jax.named_scope("barrier"):
                pl.semaphore_wait(barrier, groups)
        with jax.named_scope("start_r"):
            if turn == 0:
                order = [(plane, n) for n in range(2) for plane in (far_a, far_b)]
            else:
                order = [(py, n) for n in range(1, along_z)]
                order += [(sibling, 0), (sibling, 1)]
                order += [(plane, n) for n in range(2, along_z) for plane in (far_a, far_b, sibling)]
            for plane, n in order:
                copy_r(to(plane, n), me).start()
    recv_r[me] = send_r[me]

    for turn in range(2):
        first = (1 - side if turn == 0 else side) * half
        with jax.named_scope(f"gated_l{turn}"):
            value = gated(0, first, 0, flat_m)
            for part in range(half_groups):
                send_l[first // gc + part] = value[part * gc : (part + 1) * gc].astype(jnp.bfloat16)
        with jax.named_scope("start_l"):
            if turn == 0:
                order = [(plane, n) for n in range(2) for plane in (far_a, far_b)]
            else:
                order = [(py, n) for n in range(1, along_z)]
                order += [(sibling, 0), (sibling, 1)]
                order += [(plane, n) for n in range(2, along_z) for plane in (far_a, far_b, sibling)]
            for plane, n in order:
                copy_l(to(plane, n), me, n).start()
    recv_l[me] = send_l[me]

    with jax.named_scope("gate"):
        loads[3].wait()
        loads[4].wait()
        gate_f32[...] = 0.5 + 0.5 * jnp.tanh(
            0.5 * jnp.dot(normed_bf[...], gate_ref[...], preferred_element_type=jnp.float32)
        )

    lane8 = lax.broadcasted_iota(jnp.int32, (gc, LANES), 1)

    def lanes_from(value, start):
        block = value[:, start // LANES * LANES : start // LANES * LANES + LANES]
        shift = start % LANES
        return block if shift == 0 else pltpu.roll(block, LANES - shift, 1)

    def spread_main(value, s, target):
        for k in range(cols):
            at = pl.multiple_of((s * cols + k) * gc, gc)
            target[pl.ds(at, gc), :] = lanes_from(value, k * main)

    def spread_edge(value, s):
        for k in range(cols):
            at = pl.multiple_of((s * cols + k) * gc, gc)
            edge_s[pl.ds(at, gc), :] = lanes_from(value, flat + k * edge)

    def spread_right(value, s, target):
        for k in range(cols):
            at = pl.multiple_of((s * cols + k) * gc, gc)
            begin = flat_m + k * edge
            block = value[:, begin // LANES * LANES : begin // LANES * LANES + LANES]
            shift = (main - begin) % LANES
            block = block if shift == 0 else pltpu.roll(block, shift, 1)
            target[pl.ds(at, gc), :] = jnp.where(lane8 < main, lanes_from(value, k * main), block)

    planes = (py, far_a, far_b, sibling)

    def take_r(n, carry):
        for plane in planes:
            s = source(plane, n)

            @pl.when(s != me)
            def _():
                copy_r(s, s).wait_recv()

            copy_x(s).start()
        for plane in planes:
            s = source(plane, n)
            value = recv_r[s].astype(jnp.float32)
            spread_right(value, s, right_s.at[px])
            spread_edge(value, s)
        return carry

    with jax.named_scope("take_r"):
        lax.fori_loop(0, along_z, take_r, 0)

    def take_x(n, carry):
        pltpu.make_async_remote_copy(
            src_ref=recv_r.at[0:along_y, :, 0:wide], dst_ref=recv_x.at[0:along_y],
            send_sem=send_sem.at[1], recv_sem=rsem_x.at[n], device_id=partner,
            device_id_type=MESH,
        ).wait_recv()
        for plane in planes:
            s = source(plane, n)
            spread_right(recv_x[s].astype(jnp.float32), s, right_s.at[1 - px])
        return carry

    with jax.named_scope("take_x"):
        lax.fori_loop(0, along_z, take_x, 0)

    def tri(left, width, c, first):
        for h in range(2):
            if first:
                right = right_s[h, pl.ds(c, residues, stride=gc), :].astype(jnp.bfloat16)
                right_bf[h, c] = right
            else:
                right = right_bf[h, c]
            block = lax.dot_general(
                right[:, 0:rows], left[:, 0:width], (((0,), (0,)), ((), ())),
                preferred_element_type=jnp.float32,
            )
            tri_s[pl.ds(h * rows * gc + c, rows, stride=gc), 0:width] = block

    def pack(d, width):
        pieces = []
        per = LANES // width
        for begin in range(0, cols, per):
            total = None
            for n in range(min(per, cols - begin)):
                at = pl.multiple_of((d * cols + begin + n) * gc, gc)
                piece = tri_s[pl.ds(at, gc), :]
                piece = piece if n == 0 else pltpu.roll(piece, n * width, 1)
                total = piece if n == 0 else jnp.where(lane8 < n * width, total, piece)
            pieces.append(total)
        return jnp.concatenate(pieces, axis=1).astype(jnp.bfloat16)

    def ship(width, buffer, landed, copy):
        def around(n, carry):
            goals = [to(plane, n) for plane in (far_a, far_b, sibling, py)]
            packed = [pack(d, width) for d in goals]
            for d, value in zip(goals, packed):
                buffer[d] = value
            for d in goals:

                @pl.when(d != me)
                def _():
                    copy(d, me).start()

            return carry

        lax.fori_loop(0, along_z, around, 0)
        landed[me] = buffer[me]

    with jax.named_scope("tri_e"):
        for c in range(gc):
            left = edge_s[pl.ds(c, residues, stride=gc), :].astype(jnp.bfloat16)
            tri(left, edge, c, True)
    with jax.named_scope("ship_e"):
        ship(edge, send_e, recv_e, copy_e)

    def take_l(n, carry):
        @pl.when(n == 0)
        def _():
            copy_l(0, 0, 0, along_y - 1).wait_recv()

        @pl.when(n > 0)
        def _():
            copy_l(0, 0, n, along_y).wait_recv()

        for plane in planes:
            s = source(plane, n)
            spread_main(recv_l[s].astype(jnp.float32), s, left_s)
        return carry

    with jax.named_scope("take_l"):
        lax.fori_loop(0, along_z, take_l, 0)
    with jax.named_scope("tri_m"):
        for c in range(gc):
            left = left_s[pl.ds(c, residues, stride=gc), :].astype(jnp.bfloat16)
            tri(left, main, c, False)
    with jax.named_scope("ship_m"):
        ship(main, send_b, recv_b, copy_b)

    def final(received, low, width):
        count = width * cols
        triangle = received[:, :, 0:count].astype(jnp.float32).reshape(hidden, count)
        normed_tri = layer_norm_lead(triangle).astype(jnp.bfloat16)
        mixed = lax.dot_general(
            normed_tri, out_w_ref[...], (((0,), (0,)), ((), ())),
            preferred_element_type=jnp.float32,
        )
        first = 0 if low == 0 else flat_m
        update = (gate_f32[first : first + count] * mixed).astype(jnp.bfloat16)
        for j in range(cols):
            out_ref[j, low : low + width] = update[j * width : (j + 1) * width]

    with jax.named_scope("take_e"):
        copy_e(0, 0, groups - 1).wait_recv()
    with jax.named_scope("final_e"):
        final(recv_e, main, edge)
    with jax.named_scope("finish"):
        pltpu.make_async_remote_copy(
            src_ref=send_r.at[0 : groups - 1], dst_ref=recv_r.at[0 : groups - 1],
            send_sem=send_sem.at[0], recv_sem=rsem_r.at[0], device_id=partner,
            device_id_type=MESH,
        ).wait_send()
        copy_x(0, groups).wait_send()
        copy_l(0, 0, 0, groups - 1).wait_send()
        copy_e(0, 0, groups - 1).wait_send()
    with jax.named_scope("take_b"):
        copy_b(0, 0, groups - 1).wait_recv()
    with jax.named_scope("final_m"):
        final(recv_b, 0, main)
    with jax.named_scope("finish_b"):
        copy_b(0, 0, groups - 1).wait_send()


def scratch_list(main, rows, cols, chans, hidden, groups, residues):
    gc = hidden // groups
    flat_m, flat_e = main * cols, (rows - main) * cols
    wide = up(flat_m + flat_e, LANES)
    both = up(flat_m + 2 * flat_e, LANES)
    bf, f32 = jnp.bfloat16, jnp.float32
    return [
        ((cols, rows, chans), bf),
        ((1, residues), jnp.int32),
        ((chans, 4 * hidden), bf),
        ((chans, chans), bf),
        ((hidden, chans), bf),
        ((4 * hidden, chans), bf),
        ((rows * cols, chans), bf),
        ((rows * cols, chans), bf),
        ((rows * cols, chans), f32),
        ((groups, gc, both), bf),
        ((groups, gc, both), bf),
        ((groups, gc, wide), bf),
        ((groups, gc, flat_m), bf),
        ((groups, gc, flat_m), bf),
        ((residues * gc, LANES), f32),
        ((residues * gc, LANES), f32),
        ((2, residues * gc, LANES), f32),
        ((2, gc, residues, LANES), bf),
        ((residues * gc, LANES), f32),
        ((groups, gc, up(flat_e, LANES)), bf),
        ((groups, gc, up(flat_e, LANES)), bf),
        ((groups, gc, flat_m), bf),
        ((groups, gc, flat_m), bf),
    ]


def fits_kernel(sizes, rows, cols, chans, hidden, residues):
    groups = sizes["gy"] * sizes["gz"]
    main = rows // HALF_LANES * HALF_LANES
    edge = rows - main
    if sizes["gx"] != 2 or hidden % (4 * groups) or hidden // groups != 8:
        return False
    if sizes["gy"] != 4 or residues != 2 * rows or residues != groups * cols:
        return False
    if chans != LANES or main != HALF_LANES or edge != 16 or cols % 2:
        return False
    total = 0
    for shape, kind in scratch_list(main, rows, cols, chans, hidden, groups, residues):
        count = 1
        for extent in shape:
            count *= extent
        total += count * jnp.dtype(kind).itemsize
    return total < VMEM_BUDGET // 3


def local_fused(sizes, pair_map, residue_mask, proj_weight, gate_weight, out_weight):
    rows, cols, chans = pair_map.shape
    hidden = out_weight.shape[0]
    residues = residue_mask.shape[0]
    if not fits_kernel(sizes, rows, cols, chans, hidden, residues):
        return local(pair_map, residue_mask, proj_weight, gate_weight, out_weight)
    groups = sizes["gy"] * sizes["gz"]
    main = rows // HALF_LANES * HALF_LANES
    dma = pltpu.SemaphoreType.DMA
    vmem = pl.BlockSpec(memory_space=pltpu.VMEM)
    turned = pl.pallas_call(
        functools.partial(fused_kernel, sizes["gy"], sizes["gz"], main),
        out_shape=pltpu.VMEM((cols, rows, chans), jnp.bfloat16),
        in_specs=[pl.BlockSpec(memory_space=pltpu.HBM)] * 5,
        out_specs=vmem,
        scratch_shapes=[
            pltpu.VMEM(shape, kind)
            for shape, kind in scratch_list(main, rows, cols, chans, hidden, groups, residues)
        ]
        + [dma((5,)), dma((5,)), dma((groups,)), dma((sizes["gz"],)), dma((sizes["gz"],)), dma((2,))],
        compiler_params=pltpu.CompilerParams(
            collective_id=0, has_side_effects=True, vmem_limit_bytes=VMEM_ALL - 204800
        ),
    )(
        pair_map.transpose(1, 0, 2), residue_mask.reshape(1, residues),
        proj_weight, gate_weight, out_weight,
    )
    return turned.transpose(1, 0, 2)


def solution(mesh):
    placed = (P("gx", ("gy", "gz"), None), P(), P(), P(), P())
    return jax.shard_map(
        functools.partial(local_fused, dict(mesh.shape)), mesh=mesh, in_specs=placed, out_specs=P("gx", ("gy", "gz"), None), check_vma=False
    )
```

```python
import functools

import jax
import jax.numpy as jnp
from jax import lax
from jax.experimental import pallas as pl
from jax.experimental.pallas import tpu as pltpu
from jax.sharding import PartitionSpec as P

epsilon = 1.0


def partner_2(x, axis, bit):
    return lax.ppermute(x, axis, [(i, i ^ 1 << bit) for i in range(lax.axis_size(axis))])


def layer_norm_lead(values):
    average = jnp.mean(values, axis=0, keepdims=True)
    centred = values - average
    variance = jnp.mean(centred * centred, axis=0, keepdims=True)
    return centred * lax.rsqrt(variance + epsilon)


def layer_norm_last(values):
    average = jnp.mean(values, axis=-1, keepdims=True)
    centred = values - average
    variance = jnp.mean(centred * centred, axis=-1, keepdims=True)
    return centred * lax.rsqrt(variance + epsilon)


def swap_with(values, bit):
    return partner_2(values, "gx", bit)


def pair_join(values, bit, position):
    partner = swap_with(values, bit)
    mine_first = position // 2**bit % 2 == 0
    return jnp.where(
        mine_first,
        jnp.concatenate([values, partner], axis=1),
        jnp.concatenate([partner, values], axis=1),
    )


def whole_channels(gathered, out_weight, gate_value):
    hidden, row_count, col_count = gathered.shape
    normed_tri = layer_norm_lead(gathered.astype(jnp.float32)).astype(jnp.bfloat16)
    mixed_out = lax.dot_general(
        normed_tri.reshape(hidden, row_count * col_count),
        out_weight,
        (((0,), (0,)), ((), ())),
        preferred_element_type=jnp.float32,
    )
    return gate_value * mixed_out.reshape(row_count, col_count, out_weight.shape[1])


def local(pair_map, residue_mask, proj_weight, gate_weight, out_weight):
    row_count, col_count, chan_count = pair_map.shape
    hidden = out_weight.shape[0]
    residues = residue_mask.shape[0]
    along_x = lax.axis_size("gx")
    along_y = lax.axis_size("gy")
    along_z = lax.axis_size("gz")
    mask_float = residue_mask.astype(jnp.float32)
    row_mask = lax.dynamic_slice_in_dim(mask_float, lax.axis_index("gx") * row_count, row_count)
    col_mask = lax.dynamic_slice_in_dim(
        mask_float, (lax.axis_index("gy") * along_z + lax.axis_index("gz")) * col_count, col_count
    )
    normed = layer_norm_last(pair_map.astype(jnp.float32)).astype(jnp.bfloat16)
    flattened = normed.reshape(row_count * col_count, chan_count)
    projected = lax.dot_general(
        proj_weight, flattened, (((0,), (1,)), ((), ())), preferred_element_type=jnp.float32
    ).reshape(4 * hidden, row_count, col_count)
    pair_mask = (row_mask[:, None] * col_mask[None, :])[None, :, :]
    left_proj = (
        jax.nn.sigmoid(projected[:hidden]) * projected[hidden : 2 * hidden] * pair_mask
    ).astype(jnp.bfloat16)
    right_proj = (
        jax.nn.sigmoid(projected[2 * hidden : 3 * hidden]) * projected[3 * hidden :] * pair_mask
    ).astype(jnp.bfloat16)
    gate_value = jax.nn.sigmoid(
        jnp.dot(flattened, gate_weight, preferred_element_type=jnp.float32)
    ).reshape(row_count, col_count, chan_count)
    group_count = along_y * along_z
    group_chan = hidden // group_count
    left_group, right_group = (
        lax.all_to_all(left_proj, ("gy", "gz"), split_axis=0, concat_axis=2, tiled=True),
        lax.all_to_all(right_proj, ("gy", "gz"), split_axis=0, concat_axis=2, tiled=True),
    )
    levels = along_x.bit_length() - 1
    low_bits = levels // 2
    high_count = 2 ** (levels - low_bits)
    low_count = 2**low_bits
    position = lax.axis_index("gx")
    left_tile = left_group
    for bit in range(low_bits):
        left_tile = pair_join(left_tile, bit, position)
    right_tile = right_group
    for bit in range(low_bits, levels):
        right_tile = pair_join(right_tile, bit, position)
    block_tile = jnp.einsum(
        "cik,cjk->cij", left_tile, right_tile, preferred_element_type=jnp.float32
    ).astype(jnp.bfloat16)
    for bit in range(low_bits):
        current = block_tile.shape[1]
        span = block_tile.shape[2]
        shaped = block_tile.reshape(group_chan, current // (2 * row_count), 2, row_count, span)
        own_bit = position // 2**bit % 2
        kept = lax.dynamic_index_in_dim(shaped, own_bit, axis=2, keepdims=False).reshape(
            group_chan, current // 2, span
        )
        sent = lax.dynamic_index_in_dim(shaped, 1 - own_bit, axis=2, keepdims=False).reshape(
            group_chan, current // 2, span
        )
        arrived = swap_with(sent, bit)
        block_tile = jnp.where(
            own_bit == 0,
            jnp.concatenate([kept, arrived], axis=2),
            jnp.concatenate([arrived, kept], axis=2),
        )
    block_tile = (
        block_tile.reshape(group_chan, row_count, low_count, high_count, row_count)
        .transpose(0, 1, 3, 2, 4)
        .reshape(group_chan, row_count, residues)
    )
    gathered = lax.all_to_all(block_tile, ("gy", "gz"), split_axis=2, concat_axis=0, tiled=True)
    update = whole_channels(gathered, out_weight, gate_value)
    return update.astype(jnp.bfloat16)


MESH = pl.DeviceIdType.MESH
LANES = 128
HALF_LANES = 64
VMEM_ALL = 67043328
VMEM_BUDGET = 48 * 2**20


def up(value, step):
    return -(-value // step) * step


def gate_by(gate, value):
    return (0.5 * value) * (1.0 + jnp.tanh(0.5 * gate))


def fused_kernel(
    along_y, along_z, main,
    pair_hbm, mask_hbm, proj_hbm, gate_hbm, out_w_hbm, out_ref,
    pair_ref, mask_ref, proj_ref, gate_ref, out_w_ref,
    proj_s, normed_bf, masked_bf, gate_f32, send_r, recv_r, recv_x, send_l, recv_l,
    left_s, edge_s, edge_bf, right_s, right_bf, tri_s, send_e, recv_e, send_b, recv_b,
    load_sem, send_sem, rsem_r, rsem_x, rsem_l, rsem_b,
):
    cols, rows, chans = pair_ref.shape
    hidden = out_w_ref.shape[0]
    groups = along_y * along_z
    gc = hidden // groups
    edge = rows - main
    flat_m, flat_e = main * cols, edge * cols
    flat = flat_m + flat_e
    wide = up(flat, LANES)
    both = up(flat + flat_e, LANES)
    residues = mask_ref.shape[1]
    px, py, pz = lax.axis_index("gx"), lax.axis_index("gy"), lax.axis_index("gz")
    me = py * along_z + pz
    side = py // (along_y // 2)
    middle = along_y // 2

    def place(d):
        return (px, d // along_z, d % along_z)

    far_a, far_b = (1 - side) * middle, (1 - side) * middle + 1
    sibling = side * middle + (py + 1) % middle

    def to(plane, n):
        return plane * along_z + (pz + n) % along_z

    def source(plane, n):
        return plane * along_z + (pz + along_z - n) % along_z

    def turn_of(s):
        return (pz + along_z - s % along_z) % along_z

    partner = (1 - px, py, pz)
    barrier = pltpu.get_barrier_semaphore()

    def greet(o, carry):
        pl.semaphore_signal(barrier, inc=1, device_id=place((me + o) % groups), device_id_type=MESH)
        return carry

    with jax.named_scope("greet"):
        lax.fori_loop(1, groups, greet, 0)
        pl.semaphore_signal(barrier, inc=1, device_id=partner, device_id_type=MESH)

    loads = [
        pltpu.make_async_copy(source, target, load_sem.at[n])
        for n, (source, target) in enumerate(
            (
                (pair_hbm, pair_ref), (mask_hbm, mask_ref), (proj_hbm, proj_ref),
                (gate_hbm, gate_ref), (out_w_hbm, out_w_ref),
            )
        )
    ]
    for load in loads:
        load.start()
    with jax.named_scope("waitload"):
        loads[1].wait()
        loads[2].wait()
        proj_s[...] = proj_ref[...].astype(jnp.float32).T.astype(jnp.bfloat16)
        loads[0].wait()

    with jax.named_scope("norm"):
        mask_f = mask_ref[...].astype(jnp.float32)
        lane = lax.broadcasted_iota(jnp.int32, (rows, residues), 1)
        sub = lax.broadcasted_iota(jnp.int32, (rows, residues), 0)
        row_mask = jnp.sum(jnp.where(lane == sub + px * rows, mask_f, 0.0), axis=1, keepdims=True)
        lane_row = lax.broadcasted_iota(jnp.int32, (1, residues), 1)
        for k in range(cols):
            col_mask = jnp.sum(
                jnp.where(lane_row == me * cols + k, mask_f, 0.0), axis=1, keepdims=True
            )
            normed = layer_norm_last(pair_ref[k].astype(jnp.float32)).astype(jnp.bfloat16)
            masked = (normed.astype(jnp.float32) * (row_mask * col_mask)).astype(jnp.bfloat16)
            for target, value in ((normed_bf, normed), (masked_bf, masked)):
                target[k * main : (k + 1) * main, :] = value[0:main]
                target[flat_m + k * edge : flat_m + (k + 1) * edge, :] = value[main:rows]

    half = hidden // 2
    half_groups = groups // 2

    def gated(base, first, low, high):
        rows_of = jnp.concatenate(
            [
                proj_s[pl.ds(pl.multiple_of(base + first, half), half), :],
                proj_s[pl.ds(pl.multiple_of(base + hidden + first, half), half), :],
            ],
            axis=0,
        )
        value = lax.dot_general(
            rows_of, masked_bf[low:high, :], (((1,), (1,)), ((), ())),
            preferred_element_type=jnp.float32,
        )
        return gate_by(value[0:half], value[half:])

    def copy_r(d, slot):
        return pltpu.make_async_remote_copy(
            src_ref=send_r.at[d, :, 0:wide], dst_ref=recv_r.at[slot, :, 0:wide],
            send_sem=send_sem.at[0], recv_sem=rsem_r.at[slot], device_id=place(d),
            device_id_type=MESH,
        )

    def copy_rest(d, slot, n, count=1):
        return pltpu.make_async_remote_copy(
            src_ref=send_r.at[pl.ds(d, count), :, wide:both],
            dst_ref=recv_r.at[pl.ds(slot, count), :, wide:both],
            send_sem=send_sem.at[5], recv_sem=rsem_l.at[n + along_z], device_id=place(d),
            device_id_type=MESH,
        )

    def copy_x(s, count=1):
        return pltpu.make_async_remote_copy(
            src_ref=recv_r.at[pl.ds(s, count), :, 0:wide], dst_ref=recv_x.at[pl.ds(s, count)],
            send_sem=send_sem.at[1], recv_sem=rsem_x.at[turn_of(s)],
            device_id=partner, device_id_type=MESH,
        )

    def copy_many(source, target, kind, recv_sem, d, slot, count=1):
        return pltpu.make_async_remote_copy(
            src_ref=source.at[pl.ds(d, count)], dst_ref=target.at[pl.ds(slot, count)],
            send_sem=send_sem.at[kind], recv_sem=recv_sem, device_id=place(d),
            device_id_type=MESH,
        )

    def copy_l(d, slot, n, count=1):
        return copy_many(send_l, recv_l, 2, rsem_l.at[n], d, slot, count)

    def copy_e(d, slot, count=1):
        return copy_many(send_e, recv_e, 3, rsem_b.at[0], d, slot, count)

    def copy_b(d, slot, count=1):
        return copy_many(send_b, recv_b, 4, rsem_b.at[1], d, slot, count)

    for turn in range(2):
        first = (1 - side if turn == 0 else side) * half
        with jax.named_scope(f"gated_r{turn}"):
            value = gated(2 * hidden, first, 0, flat)
            extra = gated(0, first, flat_m, flat)
            value = jnp.concatenate([value, extra], axis=1)
            for part in range(half_groups):
                send_r[first // gc + part, :, 0 : flat + flat_e] = value[
                    part * gc : (part + 1) * gc
                ].astype(jnp.bfloat16)
        if turn == 0:
            with jax.named_scope("barrier"):
                pl.semaphore_wait(barrier, groups)
        with jax.named_scope("start_r"):
            if turn == 0:
                order = [(plane, n) for n in range(2) for plane in (far_a, far_b)]
            else:
                order = [(py, n) for n in range(1, along_z)]
                order += [(sibling, 0), (sibling, 1)]
                order += [(plane, n) for n in range(2, along_z) for plane in (far_a, far_b, sibling)]
            for plane, n in order:
                copy_r(to(plane, n), me).start()
            if turn == 1:
                for n in range(along_z):
                    for plane in (far_a, far_b, sibling, py):
                        if n == 0 and plane is py:
                            continue
                        copy_rest(to(plane, n), me, n).start()
    recv_r[me] = send_r[me]

    for turn in range(2):
        first = (1 - side if turn == 0 else side) * half
        with jax.named_scope(f"gated_l{turn}"):
            value = gated(0, first, 0, flat_m)
            for part in range(half_groups):
                send_l[first // gc + part] = value[part * gc : (part + 1) * gc].astype(jnp.bfloat16)
    recv_l[me] = send_l[me]

    with jax.named_scope("gate"):
        loads[3].wait()
        loads[4].wait()
        gate_f32[...] = 0.5 + 0.5 * jnp.tanh(
            0.5 * jnp.dot(normed_bf[...], gate_ref[...], preferred_element_type=jnp.float32)
        )

    lane8 = lax.broadcasted_iota(jnp.int32, (gc, LANES), 1)

    def lanes_from(value, start):
        block = value[:, start // LANES * LANES : start // LANES * LANES + LANES]
        shift = start % LANES
        return block if shift == 0 else pltpu.roll(block, LANES - shift, 1)

    def spread_main(value, s, target):
        for k in range(cols):
            at = pl.multiple_of((s * cols + k) * gc, gc)
            target[pl.ds(at, gc), :] = lanes_from(value, k * main)

    def spread_right(value, s, target):
        for k in range(cols):
            at = pl.multiple_of((s * cols + k) * gc, gc)
            begin = flat_m + k * edge
            block = value[:, begin // LANES * LANES : begin // LANES * LANES + LANES]
            shift = (main - begin) % LANES
            block = block if shift == 0 else pltpu.roll(block, shift, 1)
            target[pl.ds(at, gc), :] = jnp.where(lane8 < main, lanes_from(value, k * main), block)

    planes = (py, far_a, far_b, sibling)

    def forward(s):
        @pl.when(s != me)
        def _():
            copy_r(s, s).wait_recv()

        copy_x(s).start()

    def spread_r(s):
        value = recv_r[s, :, 0:wide].astype(jnp.float32)
        spread_right(value, s, right_s.at[px])

    def take_r(n, carry):
        for plane in planes[1:]:
            forward(source(plane, n))
        for plane in planes[1:]:
            spread_r(source(plane, n))
        return carry

    def start_l(n, carry):
        for plane in (far_a, far_b, sibling, py):
            d = to(plane, n)

            @pl.when(d != me)
            def _():
                copy_l(d, me, n).start()

        return carry

    with jax.named_scope("take_own"):
        for n in range(along_z):
            forward(source(py, n))
        for n in range(along_z):
            spread_r(source(py, n))
    with jax.named_scope("take_r"):
        lax.fori_loop(0, 2, take_r, 0)
    with jax.named_scope("start_l"):
        lax.fori_loop(0, along_z, start_l, 0)
    with jax.named_scope("take_r"):
        lax.fori_loop(2, along_z, take_r, 0)

    def take_rest(n, carry):
        @pl.when(n == 0)
        def _():
            copy_rest(0, 0, 0, along_y - 1).wait_recv()

        @pl.when(n > 0)
        def _():
            copy_rest(0, 0, n, along_y).wait_recv()

        for plane in planes:
            s = source(plane, n)
            value = recv_r[s, :, flat_m:both].astype(jnp.float32)
            for k in range(cols):
                at = pl.multiple_of((s * cols + k) * gc, gc)
                edge_s[pl.ds(at, gc), :] = lanes_from(value, flat_e + k * edge)
        return carry

    with jax.named_scope("take_rest"):
        lax.fori_loop(0, along_z, take_rest, 0)

    def tri(left, width, c, h, first):
        if first:
            right = right_s[h, pl.ds(c, residues, stride=gc), :].astype(jnp.bfloat16)
            right_bf[h, c] = right
        else:
            right = right_bf[h, c]
        block = lax.dot_general(
            right[:, 0:rows], left[:, 0:width], (((0,), (0,)), ((), ())),
            preferred_element_type=jnp.float32,
        )
        at = pl.multiple_of(h * rows * gc, gc)
        tri_s[pl.ds(at + c, rows, stride=gc), 0:width] = block

    with jax.named_scope("tri_own"):
        for c in range(gc):
            left = edge_s[pl.ds(c, residues, stride=gc), :].astype(jnp.bfloat16)
            edge_bf[c] = left
            tri(left, edge, c, px, True)

    def take_x(n, carry):
        pltpu.make_async_remote_copy(
            src_ref=recv_r.at[0:along_y, :, 0:wide], dst_ref=recv_x.at[0:along_y],
            send_sem=send_sem.at[1], recv_sem=rsem_x.at[n], device_id=partner,
            device_id_type=MESH,
        ).wait_recv()
        for plane in planes:
            s = source(plane, n)
            spread_right(recv_x[s].astype(jnp.float32), s, right_s.at[1 - px])
        return carry

    with jax.named_scope("take_x"):
        lax.fori_loop(0, along_z, take_x, 0)

    def pack(d, width):
        pieces = []
        per = LANES // width
        for begin in range(0, cols, per):
            total = None
            for n in range(min(per, cols - begin)):
                at = pl.multiple_of((d * cols + begin + n) * gc, gc)
                piece = tri_s[pl.ds(at, gc), :]
                piece = piece if n == 0 else pltpu.roll(piece, n * width, 1)
                total = piece if n == 0 else jnp.where(lane8 < n * width, total, piece)
            pieces.append(total)
        return jnp.concatenate(pieces, axis=1).astype(jnp.bfloat16)

    def ship(width, buffer, landed, copy):
        def around(n, carry):
            goals = [to(plane, n) for plane in (far_a, far_b, sibling, py)]
            packed = [pack(d, width) for d in goals]
            for d, value in zip(goals, packed):
                buffer[d] = value
            for d in goals:

                @pl.when(d != me)
                def _():
                    copy(d, me).start()

            return carry

        lax.fori_loop(0, along_z, around, 0)
        landed[me] = buffer[me]

    with jax.named_scope("tri_e"):
        for c in range(gc):
            tri(edge_bf[c], edge, c, 1 - px, True)
    with jax.named_scope("ship_e"):
        ship(edge, send_e, recv_e, copy_e)

    def take_l(n, carry):
        @pl.when(n == 0)
        def _():
            copy_l(0, 0, 0, along_y - 1).wait_recv()

        @pl.when(n > 0)
        def _():
            copy_l(0, 0, n, along_y).wait_recv()

        for plane in planes:
            s = source(plane, n)
            spread_main(recv_l[s].astype(jnp.float32), s, left_s)
        return carry

    with jax.named_scope("take_l"):
        lax.fori_loop(0, along_z, take_l, 0)
    with jax.named_scope("tri_m"):
        for c in range(gc):
            left = left_s[pl.ds(c, residues, stride=gc), :].astype(jnp.bfloat16)
            for h in range(2):
                tri(left, main, c, h, False)
    with jax.named_scope("ship_m"):
        ship(main, send_b, recv_b, copy_b)

    def final(received, low, width):
        count = width * cols
        triangle = received[:, :, 0:count].astype(jnp.float32).reshape(hidden, count)
        normed_tri = layer_norm_lead(triangle).astype(jnp.bfloat16)
        mixed = lax.dot_general(
            normed_tri, out_w_ref[...], (((0,), (0,)), ((), ())),
            preferred_element_type=jnp.float32,
        )
        first = 0 if low == 0 else flat_m
        update = (gate_f32[first : first + count] * mixed).astype(jnp.bfloat16)
        for j in range(cols):
            out_ref[j, low : low + width] = update[j * width : (j + 1) * width]

    with jax.named_scope("take_e"):
        copy_e(0, 0, groups - 1).wait_recv()
    with jax.named_scope("final_e"):
        final(recv_e, main, edge)
    with jax.named_scope("finish"):
        pltpu.make_async_remote_copy(
            src_ref=send_r.at[0 : groups - 1, :, 0:wide],
            dst_ref=recv_r.at[0 : groups - 1, :, 0:wide],
            send_sem=send_sem.at[0], recv_sem=rsem_r.at[0], device_id=partner,
            device_id_type=MESH,
        ).wait_send()
        copy_rest(0, 0, 0, groups - 1).wait_send()
        copy_x(0, groups).wait_send()
        copy_l(0, 0, 0, groups - 1).wait_send()
        copy_e(0, 0, groups - 1).wait_send()
    with jax.named_scope("take_b"):
        copy_b(0, 0, groups - 1).wait_recv()
    with jax.named_scope("final_m"):
        final(recv_b, 0, main)
    with jax.named_scope("finish_b"):
        copy_b(0, 0, groups - 1).wait_send()


def scratch_list(main, rows, cols, chans, hidden, groups, residues):
    gc = hidden // groups
    flat_m, flat_e = main * cols, (rows - main) * cols
    wide = up(flat_m + flat_e, LANES)
    both = up(flat_m + 2 * flat_e, LANES)
    bf, f32 = jnp.bfloat16, jnp.float32
    return [
        ((cols, rows, chans), bf),
        ((1, residues), jnp.int32),
        ((chans, 4 * hidden), bf),
        ((chans, chans), bf),
        ((hidden, chans), bf),
        ((4 * hidden, chans), bf),
        ((rows * cols, chans), bf),
        ((rows * cols, chans), bf),
        ((rows * cols, chans), f32),
        ((groups, gc, both), bf),
        ((groups, gc, both), bf),
        ((groups, gc, wide), bf),
        ((groups, gc, flat_m), bf),
        ((groups, gc, flat_m), bf),
        ((residues * gc, LANES), f32),
        ((residues * gc, LANES), f32),
        ((gc, residues, LANES), bf),
        ((2, residues * gc, LANES), f32),
        ((2, gc, residues, LANES), bf),
        ((residues * gc, LANES), f32),
        ((groups, gc, up(flat_e, LANES)), bf),
        ((groups, gc, up(flat_e, LANES)), bf),
        ((groups, gc, flat_m), bf),
        ((groups, gc, flat_m), bf),
    ]


def fits_kernel(sizes, rows, cols, chans, hidden, residues):
    groups = sizes["gy"] * sizes["gz"]
    main = rows // HALF_LANES * HALF_LANES
    edge = rows - main
    if sizes["gx"] != 2 or hidden % (4 * groups) or hidden // groups != 8:
        return False
    if sizes["gy"] != 4 or residues != 2 * rows or residues != groups * cols:
        return False
    if chans != LANES or main != HALF_LANES or edge != 16 or cols % 2:
        return False
    total = 0
    for shape, kind in scratch_list(main, rows, cols, chans, hidden, groups, residues):
        count = 1
        for extent in shape:
            count *= extent
        total += count * jnp.dtype(kind).itemsize
    return total < VMEM_BUDGET // 3


def local_fused(sizes, pair_map, residue_mask, proj_weight, gate_weight, out_weight):
    rows, cols, chans = pair_map.shape
    hidden = out_weight.shape[0]
    residues = residue_mask.shape[0]
    if not fits_kernel(sizes, rows, cols, chans, hidden, residues):
        return local(pair_map, residue_mask, proj_weight, gate_weight, out_weight)
    groups = sizes["gy"] * sizes["gz"]
    main = rows // HALF_LANES * HALF_LANES
    dma = pltpu.SemaphoreType.DMA
    vmem = pl.BlockSpec(memory_space=pltpu.VMEM)
    turned = pl.pallas_call(
        functools.partial(fused_kernel, sizes["gy"], sizes["gz"], main),
        out_shape=pltpu.VMEM((cols, rows, chans), jnp.bfloat16),
        in_specs=[pl.BlockSpec(memory_space=pltpu.HBM)] * 5,
        out_specs=vmem,
        scratch_shapes=[
            pltpu.VMEM(shape, kind)
            for shape, kind in scratch_list(main, rows, cols, chans, hidden, groups, residues)
        ]
        + [dma((5,)), dma((6,)), dma((groups,)), dma((sizes["gz"],)), dma((2 * sizes["gz"],)), dma((2,))],
        compiler_params=pltpu.CompilerParams(
            collective_id=0, has_side_effects=True, vmem_limit_bytes=VMEM_ALL - 204800
        ),
    )(
        pair_map.transpose(1, 0, 2), residue_mask.reshape(1, residues),
        proj_weight, gate_weight, out_weight,
    )
    return turned.transpose(1, 0, 2)


def solution(mesh):
    placed = (P("gx", ("gy", "gz"), None), P(), P(), P(), P())
    return jax.shard_map(
        functools.partial(local_fused, dict(mesh.shape)), mesh=mesh, in_specs=placed, out_specs=P("gx", ("gy", "gz"), None), check_vma=False
    )
```

```python
import functools

import jax
import jax.numpy as jnp
from jax import lax
from jax.experimental import pallas as pl
from jax.experimental.pallas import tpu as pltpu
from jax.sharding import PartitionSpec as P

epsilon = 1.0


def partner_2(x, axis, bit):
    return lax.ppermute(x, axis, [(i, i ^ 1 << bit) for i in range(lax.axis_size(axis))])


def layer_norm_lead(values):
    average = jnp.mean(values, axis=0, keepdims=True)
    centred = values - average
    variance = jnp.mean(centred * centred, axis=0, keepdims=True)
    return centred * lax.rsqrt(variance + epsilon)


def layer_norm_last(values):
    average = jnp.mean(values, axis=-1, keepdims=True)
    centred = values - average
    variance = jnp.mean(centred * centred, axis=-1, keepdims=True)
    return centred * lax.rsqrt(variance + epsilon)


def swap_with(values, bit):
    return partner_2(values, "gx", bit)


def pair_join(values, bit, position):
    partner = swap_with(values, bit)
    mine_first = position // 2**bit % 2 == 0
    return jnp.where(
        mine_first,
        jnp.concatenate([values, partner], axis=1),
        jnp.concatenate([partner, values], axis=1),
    )


def whole_channels(gathered, out_weight, gate_value):
    hidden, row_count, col_count = gathered.shape
    normed_tri = layer_norm_lead(gathered.astype(jnp.float32)).astype(jnp.bfloat16)
    mixed_out = lax.dot_general(
        normed_tri.reshape(hidden, row_count * col_count),
        out_weight,
        (((0,), (0,)), ((), ())),
        preferred_element_type=jnp.float32,
    )
    return gate_value * mixed_out.reshape(row_count, col_count, out_weight.shape[1])


def local(pair_map, residue_mask, proj_weight, gate_weight, out_weight):
    row_count, col_count, chan_count = pair_map.shape
    hidden = out_weight.shape[0]
    residues = residue_mask.shape[0]
    along_x = lax.axis_size("gx")
    along_y = lax.axis_size("gy")
    along_z = lax.axis_size("gz")
    mask_float = residue_mask.astype(jnp.float32)
    row_mask = lax.dynamic_slice_in_dim(mask_float, lax.axis_index("gx") * row_count, row_count)
    col_mask = lax.dynamic_slice_in_dim(
        mask_float, (lax.axis_index("gy") * along_z + lax.axis_index("gz")) * col_count, col_count
    )
    normed = layer_norm_last(pair_map.astype(jnp.float32)).astype(jnp.bfloat16)
    flattened = normed.reshape(row_count * col_count, chan_count)
    projected = lax.dot_general(
        proj_weight, flattened, (((0,), (1,)), ((), ())), preferred_element_type=jnp.float32
    ).reshape(4 * hidden, row_count, col_count)
    pair_mask = (row_mask[:, None] * col_mask[None, :])[None, :, :]
    left_proj = (
        jax.nn.sigmoid(projected[:hidden]) * projected[hidden : 2 * hidden] * pair_mask
    ).astype(jnp.bfloat16)
    right_proj = (
        jax.nn.sigmoid(projected[2 * hidden : 3 * hidden]) * projected[3 * hidden :] * pair_mask
    ).astype(jnp.bfloat16)
    gate_value = jax.nn.sigmoid(
        jnp.dot(flattened, gate_weight, preferred_element_type=jnp.float32)
    ).reshape(row_count, col_count, chan_count)
    group_count = along_y * along_z
    group_chan = hidden // group_count
    left_group, right_group = (
        lax.all_to_all(left_proj, ("gy", "gz"), split_axis=0, concat_axis=2, tiled=True),
        lax.all_to_all(right_proj, ("gy", "gz"), split_axis=0, concat_axis=2, tiled=True),
    )
    levels = along_x.bit_length() - 1
    low_bits = levels // 2
    high_count = 2 ** (levels - low_bits)
    low_count = 2**low_bits
    position = lax.axis_index("gx")
    left_tile = left_group
    for bit in range(low_bits):
        left_tile = pair_join(left_tile, bit, position)
    right_tile = right_group
    for bit in range(low_bits, levels):
        right_tile = pair_join(right_tile, bit, position)
    block_tile = jnp.einsum(
        "cik,cjk->cij", left_tile, right_tile, preferred_element_type=jnp.float32
    ).astype(jnp.bfloat16)
    for bit in range(low_bits):
        current = block_tile.shape[1]
        span = block_tile.shape[2]
        shaped = block_tile.reshape(group_chan, current // (2 * row_count), 2, row_count, span)
        own_bit = position // 2**bit % 2
        kept = lax.dynamic_index_in_dim(shaped, own_bit, axis=2, keepdims=False).reshape(
            group_chan, current // 2, span
        )
        sent = lax.dynamic_index_in_dim(shaped, 1 - own_bit, axis=2, keepdims=False).reshape(
            group_chan, current // 2, span
        )
        arrived = swap_with(sent, bit)
        block_tile = jnp.where(
            own_bit == 0,
            jnp.concatenate([kept, arrived], axis=2),
            jnp.concatenate([arrived, kept], axis=2),
        )
    block_tile = (
        block_tile.reshape(group_chan, row_count, low_count, high_count, row_count)
        .transpose(0, 1, 3, 2, 4)
        .reshape(group_chan, row_count, residues)
    )
    gathered = lax.all_to_all(block_tile, ("gy", "gz"), split_axis=2, concat_axis=0, tiled=True)
    update = whole_channels(gathered, out_weight, gate_value)
    return update.astype(jnp.bfloat16)


MESH = pl.DeviceIdType.MESH
LANES = 128
VMEM_ALL = 67043328
VMEM_BUDGET = 48 * 2**20


def up(value, step):
    return -(-value // step) * step


def main_rows(rows):
    return rows * 8 // 10 // 16 * 16


def gate_by(gate, value):
    return (0.5 * value) * (1.0 + jnp.tanh(0.5 * gate))


def fused_kernel(
    along_y, along_z, main,
    pair_hbm, mask_hbm, proj_hbm, gate_hbm, out_w_hbm, out_ref,
    pair_ref, mask_ref, proj_ref, gate_ref, out_w_ref,
    proj_s, normed_bf, masked_bf, gate_f32, send_r, recv_r, recv_x, send_l, recv_l,
    left_s, edge_s, edge_bf, right_s, right_bf, tri_s, send_e, recv_e, send_b, recv_b,
    load_sem, send_sem, rsem_r, rsem_x, rsem_l, rsem_b,
):
    cols, rows, chans = pair_ref.shape
    hidden = out_w_ref.shape[0]
    groups = along_y * along_z
    gc = hidden // groups
    edge = rows - main
    flat_m, flat_e = main * cols, edge * cols
    flat = flat_m + flat_e
    wide = up(flat, LANES)
    both = up(flat + flat_e, LANES)
    residues = mask_ref.shape[1]
    px, py, pz = lax.axis_index("gx"), lax.axis_index("gy"), lax.axis_index("gz")
    me = py * along_z + pz
    side = py // (along_y // 2)
    middle = along_y // 2

    def place(d):
        return (px, d // along_z, d % along_z)

    far_a = (1 - side) * (along_y - 1)
    far_b = side * (middle - 1) + (1 - side) * middle
    sibling = side * middle + (py + 1) % middle

    def to(plane, n):
        m = n if plane is py else (n + 2) % along_z
        return plane * along_z + (pz // 2 + m // 2) % (along_z // 2) * 2 + (pz + m) % 2

    partner = (1 - px, py, pz)
    barrier = pltpu.get_barrier_semaphore()

    def greet(o, carry):
        pl.semaphore_signal(barrier, inc=1, device_id=place((me + o) % groups), device_id_type=MESH)
        return carry

    with jax.named_scope("greet"):
        lax.fori_loop(1, groups, greet, 0)
        pl.semaphore_signal(barrier, inc=1, device_id=partner, device_id_type=MESH)

    loads = [
        pltpu.make_async_copy(source, target, load_sem.at[n])
        for n, (source, target) in enumerate(
            (
                (pair_hbm, pair_ref), (mask_hbm, mask_ref), (proj_hbm, proj_ref),
                (gate_hbm, gate_ref), (out_w_hbm, out_w_ref),
            )
        )
    ]
    for load in loads:
        load.start()
    with jax.named_scope("waitload"):
        loads[1].wait()
        loads[2].wait()
        proj_s[...] = proj_ref[...].astype(jnp.float32).T.astype(jnp.bfloat16)
        loads[0].wait()

    with jax.named_scope("norm"):
        mask_f = mask_ref[...].astype(jnp.float32)
        lane = lax.broadcasted_iota(jnp.int32, (rows, residues), 1)
        sub = lax.broadcasted_iota(jnp.int32, (rows, residues), 0)
        row_mask = jnp.sum(jnp.where(lane == sub + px * rows, mask_f, 0.0), axis=1, keepdims=True)
        lane_row = lax.broadcasted_iota(jnp.int32, (1, residues), 1)
        for k in range(cols):
            col_mask = jnp.sum(
                jnp.where(lane_row == me * cols + k, mask_f, 0.0), axis=1, keepdims=True
            )
            normed = layer_norm_last(pair_ref[k].astype(jnp.float32)).astype(jnp.bfloat16)
            masked = (normed.astype(jnp.float32) * (row_mask * col_mask)).astype(jnp.bfloat16)
            for target, value in ((normed_bf, normed), (masked_bf, masked)):
                target[k * main : (k + 1) * main, :] = value[0:main]
                target[flat_m + k * edge : flat_m + (k + 1) * edge, :] = value[main:rows]

    half = hidden // 2
    half_groups = groups // 2

    def gated(base, first, low, high):
        rows_of = jnp.concatenate(
            [
                proj_s[pl.ds(pl.multiple_of(base + first, half), half), :],
                proj_s[pl.ds(pl.multiple_of(base + hidden + first, half), half), :],
            ],
            axis=0,
        )
        value = lax.dot_general(
            rows_of, masked_bf[low:high, :], (((1,), (1,)), ((), ())),
            preferred_element_type=jnp.float32,
        )
        return gate_by(value[0:half], value[half:])

    def copy_r(d, slot):
        return pltpu.make_async_remote_copy(
            src_ref=send_r.at[d, :, 0:wide], dst_ref=recv_r.at[slot, :, 0:wide],
            send_sem=send_sem.at[0], recv_sem=rsem_r.at[slot], device_id=place(d),
            device_id_type=MESH,
        )

    def copy_rest(d, slot, n, count=1):
        return pltpu.make_async_remote_copy(
            src_ref=send_r.at[pl.ds(d, count), :, wide:both],
            dst_ref=recv_r.at[pl.ds(slot, count), :, wide:both],
            send_sem=send_sem.at[5], recv_sem=rsem_l.at[n + along_z], device_id=place(d),
            device_id_type=MESH,
        )

    def copy_x(s, n, count=1):
        return pltpu.make_async_remote_copy(
            src_ref=recv_r.at[pl.ds(s, count), :, 0:wide], dst_ref=recv_x.at[pl.ds(s, count)],
            send_sem=send_sem.at[1], recv_sem=rsem_x.at[n],
            device_id=partner, device_id_type=MESH,
        )

    def copy_many(source, target, kind, recv_sem, d, slot, count=1):
        return pltpu.make_async_remote_copy(
            src_ref=source.at[pl.ds(d, count)], dst_ref=target.at[pl.ds(slot, count)],
            send_sem=send_sem.at[kind], recv_sem=recv_sem, device_id=place(d),
            device_id_type=MESH,
        )

    def copy_l(d, slot, n, count=1):
        return copy_many(send_l, recv_l, 2, rsem_l.at[n], d, slot, count)

    def copy_e(d, slot, count=1):
        return copy_many(send_e, recv_e, 3, rsem_b.at[0], d, slot, count)

    def copy_b(d, slot, count=1):
        return copy_many(send_b, recv_b, 4, rsem_b.at[1], d, slot, count)

    for turn in range(2):
        first = (1 - side if turn == 0 else side) * half
        with jax.named_scope(f"gated_r{turn}"):
            value = gated(2 * hidden, first, 0, flat)
            extra = gated(0, first, flat_m, flat)
            value = jnp.concatenate([value, extra], axis=1)
            for part in range(half_groups):
                send_r[first // gc + part, :, 0 : flat + flat_e] = value[
                    part * gc : (part + 1) * gc
                ].astype(jnp.bfloat16)
        if turn == 0:
            with jax.named_scope("barrier"):
                pl.semaphore_wait(barrier, groups)
        with jax.named_scope("start_r"):
            if turn == 0:
                order = [(plane, n) for n in range(2) for plane in (far_a, far_b)]
            else:
                order = [(py, n) for n in range(1, along_z)]
                order += [(sibling, n) for n in range(along_z)]
                order += [(plane, n) for n in range(2, along_z) for plane in (far_a, far_b)]
            for plane, n in order:
                copy_r(to(plane, n), me).start()
            if turn == 1:
                for n in range(along_z):
                    for plane in (far_a, far_b, sibling, py):
                        if n == 0 and plane is py:
                            continue
                        copy_rest(to(plane, n), me, n).start()
    recv_r[me] = send_r[me]

    for turn in range(2):
        first = (1 - side if turn == 0 else side) * half
        with jax.named_scope(f"gated_l{turn}"):
            value = gated(0, first, 0, flat_m)
            for part in range(half_groups):
                send_l[first // gc + part, :, 0:flat_m] = value[
                    part * gc : (part + 1) * gc
                ].astype(jnp.bfloat16)
    recv_l[me] = send_l[me]

    with jax.named_scope("gate"):
        loads[3].wait()
        loads[4].wait()
        gate_f32[...] = 0.5 + 0.5 * jnp.tanh(
            0.5 * jnp.dot(normed_bf[...], gate_ref[...], preferred_element_type=jnp.float32)
        )

    lane8 = lax.broadcasted_iota(jnp.int32, (gc, LANES), 1)

    def lift(value, begin, width, lane):
        low, high = begin // LANES, (begin + width - 1) // LANES
        shift = (lane - begin) % LANES

        def turned(n):
            block = value[:, n * LANES : (n + 1) * LANES]
            return block if shift == 0 else pltpu.roll(block, shift, 1)

        if low == high:
            return turned(low)
        return jnp.where(lane8 < lane + high * LANES - begin, turned(low), turned(high))

    def spread_main(value, s, target):
        for k in range(cols):
            at = pl.multiple_of((s * cols + k) * gc, gc)
            target[pl.ds(at, gc), :] = lift(value, k * main, main, 0)

    def spread_right(value, s, target):
        for k in range(cols):
            at = pl.multiple_of((s * cols + k) * gc, gc)
            target[pl.ds(at, gc), :] = jnp.where(
                lane8 < main,
                lift(value, k * main, main, 0),
                lift(value, flat_m + k * edge, edge, main),
            )

    planes = (py, far_a, far_b, sibling)

    def forward(plane, n):
        s = to(plane, n)
        copy_r(s, s).wait_recv()
        copy_x(s, n).start()

    def spread_r(s):
        value = recv_r[s, :, 0:wide].astype(jnp.float32)
        spread_right(value, s, right_s.at[px])

    def take_plane(plane, first):
        for n in range(first, along_z):
            forward(plane, n)
        for n in range(along_z):
            spread_r(to(plane, n))

    def take_far(n, carry):
        for plane in (far_a, far_b):
            forward(plane, n)
        for plane in (far_a, far_b):
            spread_r(to(plane, n))
        return carry

    def start_l(n, carry):
        for plane in (far_a, far_b, sibling, py):
            d = to(plane, n)

            @pl.when(d != me)
            def _():
                copy_l(d, me, n).start()

        return carry

    copy_x(me, 0).start()
    with jax.named_scope("take_own"):
        take_plane(py, 1)
    with jax.named_scope("take_far0"):
        take_far(0, 0)
    with jax.named_scope("take_sib"):
        take_plane(sibling, 0)
    with jax.named_scope("take_far1"):
        take_far(1, 0)
    with jax.named_scope("wait_send"):
        pltpu.make_async_remote_copy(
            src_ref=send_r.at[0 : groups - 1, :, 0:wide],
            dst_ref=recv_r.at[0 : groups - 1, :, 0:wide],
            send_sem=send_sem.at[0], recv_sem=rsem_r.at[0], device_id=partner,
            device_id_type=MESH,
        ).wait_send()
    with jax.named_scope("start_l"):
        lax.fori_loop(0, along_z, start_l, 0)
    with jax.named_scope("take_far2"):
        take_far(2, 0)
    with jax.named_scope("take_far3"):
        take_far(3, 0)

    rest_low = flat // LANES * LANES

    def take_rest(n, carry):
        @pl.when(n == 0)
        def _():
            copy_rest(0, 0, 0, along_y - 1).wait_recv()

        @pl.when(n > 0)
        def _():
            copy_rest(0, 0, n, along_y).wait_recv()

        for plane in planes:
            s = to(plane, n)
            value = recv_r[s, :, rest_low:both].astype(jnp.float32)
            for k in range(cols):
                at = pl.multiple_of((s * cols + k) * gc, gc)
                edge_s[pl.ds(at, gc), :] = lift(value, flat + k * edge - rest_low, edge, 0)
        return carry

    with jax.named_scope("take_rest"):
        lax.fori_loop(0, along_z, take_rest, 0)

    def tri(left, width, c, h, first):
        if first:
            right = right_s[h, pl.ds(c, residues, stride=gc), :].astype(jnp.bfloat16)
            right_bf[h, c] = right
        else:
            right = right_bf[h, c]
        block = lax.dot_general(
            right[:, 0:rows], left[:, 0:width], (((0,), (0,)), ((), ())),
            preferred_element_type=jnp.float32,
        )
        at = pl.multiple_of(h * rows * gc, gc)
        tri_s[pl.ds(at + c, rows, stride=gc), 0:width] = block

    with jax.named_scope("tri_own"):
        for c in range(gc):
            left = edge_s[pl.ds(c, residues, stride=gc), :].astype(jnp.bfloat16)
            edge_bf[c] = left
            tri(left, edge, c, px, True)

    def take_x(n, carry):
        pltpu.make_async_remote_copy(
            src_ref=recv_r.at[0:along_y, :, 0:wide], dst_ref=recv_x.at[0:along_y],
            send_sem=send_sem.at[1], recv_sem=rsem_x.at[n], device_id=partner,
            device_id_type=MESH,
        ).wait_recv()
        for plane in planes:
            s = to(plane, n)
            spread_right(recv_x[s].astype(jnp.float32), s, right_s.at[1 - px])
        return carry

    with jax.named_scope("take_x"):
        lax.fori_loop(0, along_z, take_x, 0)

    def pack(d, width):
        blocks = [None] * (up(cols * width, LANES) // LANES)
        for j in range(cols):
            at = pl.multiple_of((d * cols + j) * gc, gc)
            shift = j * width % LANES
            piece = tri_s[pl.ds(at, gc), :]
            piece = piece if shift == 0 else pltpu.roll(piece, shift, 1)
            n = j * width // LANES
            blocks[n] = piece if shift == 0 else jnp.where(lane8 < shift, blocks[n], piece)
            if shift + width > LANES:
                blocks[n + 1] = piece
        return jnp.concatenate(blocks, axis=1).astype(jnp.bfloat16)

    def ship(width, buffer, landed, copy):
        def around(n, carry):
            goals = [to(plane, n) for plane in (far_a, far_b, sibling, py)]
            packed = [pack(d, width) for d in goals]
            for d, value in zip(goals, packed):
                buffer[d] = value
            for d in goals:

                @pl.when(d != me)
                def _():
                    copy(d, me).start()

            return carry

        lax.fori_loop(0, along_z, around, 0)
        landed[me] = buffer[me]

    with jax.named_scope("tri_e"):
        for c in range(gc):
            tri(edge_bf[c], edge, c, 1 - px, True)
    with jax.named_scope("ship_e"):
        ship(edge, send_e, recv_e, copy_e)

    def take_l(n, carry):
        @pl.when(n == 0)
        def _():
            copy_l(0, 0, 0, along_y - 1).wait_recv()

        @pl.when(n > 0)
        def _():
            copy_l(0, 0, n, along_y).wait_recv()

        for plane in planes:
            s = to(plane, n)
            spread_main(recv_l[s].astype(jnp.float32), s, left_s)
        return carry

    with jax.named_scope("take_l"):
        lax.fori_loop(0, along_z, take_l, 0)
    with jax.named_scope("tri_m"):
        for c in range(gc):
            left = left_s[pl.ds(c, residues, stride=gc), :].astype(jnp.bfloat16)
            for h in range(2):
                tri(left, main, c, h, False)
    with jax.named_scope("ship_m"):
        ship(main, send_b, recv_b, copy_b)

    def final(received, low, width):
        count = width * cols
        triangle = received[:, :, 0:count].astype(jnp.float32).reshape(hidden, count)
        normed_tri = layer_norm_lead(triangle).astype(jnp.bfloat16)
        mixed = lax.dot_general(
            normed_tri, out_w_ref[...], (((0,), (0,)), ((), ())),
            preferred_element_type=jnp.float32,
        )
        first = 0 if low == 0 else flat_m
        update = (gate_f32[first : first + count] * mixed).astype(jnp.bfloat16)
        for j in range(cols):
            out_ref[j, low : low + width] = update[j * width : (j + 1) * width]

    with jax.named_scope("take_e"):
        copy_e(0, 0, groups - 1).wait_recv()
    with jax.named_scope("final_e"):
        final(recv_e, main, edge)
    with jax.named_scope("finish"):
        copy_rest(0, 0, 0, groups - 1).wait_send()
        copy_x(0, 0, groups).wait_send()
        copy_l(0, 0, 0, groups - 1).wait_send()
        copy_e(0, 0, groups - 1).wait_send()
    with jax.named_scope("take_b"):
        copy_b(0, 0, groups - 1).wait_recv()
    with jax.named_scope("final_m"):
        final(recv_b, 0, main)
    with jax.named_scope("finish_b"):
        copy_b(0, 0, groups - 1).wait_send()


def scratch_list(main, rows, cols, chans, hidden, groups, residues):
    gc = hidden // groups
    flat_m, flat_e = main * cols, (rows - main) * cols
    wide = up(flat_m + flat_e, LANES)
    both = up(flat_m + 2 * flat_e, LANES)
    bf, f32 = jnp.bfloat16, jnp.float32
    return [
        ((cols, rows, chans), bf),
        ((1, residues), jnp.int32),
        ((chans, 4 * hidden), bf),
        ((chans, chans), bf),
        ((hidden, chans), bf),
        ((4 * hidden, chans), bf),
        ((rows * cols, chans), bf),
        ((rows * cols, chans), bf),
        ((rows * cols, chans), f32),
        ((groups, gc, both), bf),
        ((groups, gc, both), bf),
        ((groups, gc, wide), bf),
        ((groups, gc, up(flat_m, LANES)), bf),
        ((groups, gc, up(flat_m, LANES)), bf),
        ((residues * gc, LANES), f32),
        ((residues * gc, LANES), f32),
        ((gc, residues, LANES), bf),
        ((2, residues * gc, LANES), f32),
        ((2, gc, residues, LANES), bf),
        ((residues * gc, LANES), f32),
        ((groups, gc, up(flat_e, LANES)), bf),
        ((groups, gc, up(flat_e, LANES)), bf),
        ((groups, gc, up(flat_m, LANES)), bf),
        ((groups, gc, up(flat_m, LANES)), bf),
    ]


def fits_kernel(sizes, rows, cols, chans, hidden, residues):
    groups = sizes["gy"] * sizes["gz"]
    main = main_rows(rows)
    edge = rows - main
    if sizes["gx"] != 2 or hidden % (4 * groups) or hidden // groups != 8:
        return False
    if sizes["gy"] != 4 or sizes["gz"] != 4 or residues != 2 * rows or residues != groups * cols:
        return False
    if chans != LANES or rows > LANES or rows % 16 or main < 16 or edge < 16:
        return False
    total = 0
    for shape, kind in scratch_list(main, rows, cols, chans, hidden, groups, residues):
        count = 1
        for extent in shape:
            count *= extent
        total += count * jnp.dtype(kind).itemsize
    return total < VMEM_BUDGET // 3


def local_fused(sizes, pair_map, residue_mask, proj_weight, gate_weight, out_weight):
    rows, cols, chans = pair_map.shape
    hidden = out_weight.shape[0]
    residues = residue_mask.shape[0]
    if not fits_kernel(sizes, rows, cols, chans, hidden, residues):
        return local(pair_map, residue_mask, proj_weight, gate_weight, out_weight)
    groups = sizes["gy"] * sizes["gz"]
    main = main_rows(rows)
    dma = pltpu.SemaphoreType.DMA
    vmem = pl.BlockSpec(memory_space=pltpu.VMEM)
    turned = pl.pallas_call(
        functools.partial(fused_kernel, sizes["gy"], sizes["gz"], main),
        out_shape=pltpu.VMEM((cols, rows, chans), jnp.bfloat16),
        in_specs=[pl.BlockSpec(memory_space=pltpu.HBM)] * 5,
        out_specs=vmem,
        scratch_shapes=[
            pltpu.VMEM(shape, kind)
            for shape, kind in scratch_list(main, rows, cols, chans, hidden, groups, residues)
        ]
        + [dma((5,)), dma((6,)), dma((groups,)), dma((sizes["gz"],)), dma((2 * sizes["gz"],)), dma((2,))],
        compiler_params=pltpu.CompilerParams(
            collective_id=0, has_side_effects=True, vmem_limit_bytes=VMEM_ALL - 204800
        ),
    )(
        pair_map.transpose(1, 0, 2), residue_mask.reshape(1, residues),
        proj_weight, gate_weight, out_weight,
    )
    return turned.transpose(1, 0, 2)


def solution(mesh):
    placed = (P("gx", ("gy", "gz"), None), P(), P(), P(), P())
    return jax.shard_map(
        functools.partial(local_fused, dict(mesh.shape)), mesh=mesh, in_specs=placed, out_specs=P("gx", ("gy", "gz"), None), check_vma=False
    )
```

```python
import functools

import jax
import jax.numpy as jnp
from jax import lax
from jax.experimental import pallas as pl
from jax.experimental.pallas import tpu as pltpu
from jax.sharding import PartitionSpec as P

epsilon = 1.0


def partner_2(x, axis, bit):
    return lax.ppermute(x, axis, [(i, i ^ 1 << bit) for i in range(lax.axis_size(axis))])


def layer_norm_lead(values):
    average = jnp.mean(values, axis=0, keepdims=True)
    centred = values - average
    variance = jnp.mean(centred * centred, axis=0, keepdims=True)
    return centred * lax.rsqrt(variance + epsilon)


def layer_norm_last(values):
    average = jnp.mean(values, axis=-1, keepdims=True)
    centred = values - average
    variance = jnp.mean(centred * centred, axis=-1, keepdims=True)
    return centred * lax.rsqrt(variance + epsilon)


def swap_with(values, bit):
    return partner_2(values, "gx", bit)


def pair_join(values, bit, position):
    partner = swap_with(values, bit)
    mine_first = position // 2**bit % 2 == 0
    return jnp.where(
        mine_first,
        jnp.concatenate([values, partner], axis=1),
        jnp.concatenate([partner, values], axis=1),
    )


def whole_channels(gathered, out_weight, gate_value):
    hidden, row_count, col_count = gathered.shape
    normed_tri = layer_norm_lead(gathered.astype(jnp.float32)).astype(jnp.bfloat16)
    mixed_out = lax.dot_general(
        normed_tri.reshape(hidden, row_count * col_count),
        out_weight,
        (((0,), (0,)), ((), ())),
        preferred_element_type=jnp.float32,
    )
    return gate_value * mixed_out.reshape(row_count, col_count, out_weight.shape[1])


def local(pair_map, residue_mask, proj_weight, gate_weight, out_weight):
    row_count, col_count, chan_count = pair_map.shape
    hidden = out_weight.shape[0]
    residues = residue_mask.shape[0]
    along_x = lax.axis_size("gx")
    along_y = lax.axis_size("gy")
    along_z = lax.axis_size("gz")
    mask_float = residue_mask.astype(jnp.float32)
    row_mask = lax.dynamic_slice_in_dim(mask_float, lax.axis_index("gx") * row_count, row_count)
    col_mask = lax.dynamic_slice_in_dim(
        mask_float, (lax.axis_index("gy") * along_z + lax.axis_index("gz")) * col_count, col_count
    )
    normed = layer_norm_last(pair_map.astype(jnp.float32)).astype(jnp.bfloat16)
    flattened = normed.reshape(row_count * col_count, chan_count)
    projected = lax.dot_general(
        proj_weight, flattened, (((0,), (1,)), ((), ())), preferred_element_type=jnp.float32
    ).reshape(4 * hidden, row_count, col_count)
    pair_mask = (row_mask[:, None] * col_mask[None, :])[None, :, :]
    left_proj = (
        jax.nn.sigmoid(projected[:hidden]) * projected[hidden : 2 * hidden] * pair_mask
    ).astype(jnp.bfloat16)
    right_proj = (
        jax.nn.sigmoid(projected[2 * hidden : 3 * hidden]) * projected[3 * hidden :] * pair_mask
    ).astype(jnp.bfloat16)
    gate_value = jax.nn.sigmoid(
        jnp.dot(flattened, gate_weight, preferred_element_type=jnp.float32)
    ).reshape(row_count, col_count, chan_count)
    group_count = along_y * along_z
    group_chan = hidden // group_count
    left_group, right_group = (
        lax.all_to_all(left_proj, ("gy", "gz"), split_axis=0, concat_axis=2, tiled=True),
        lax.all_to_all(right_proj, ("gy", "gz"), split_axis=0, concat_axis=2, tiled=True),
    )
    levels = along_x.bit_length() - 1
    low_bits = levels // 2
    high_count = 2 ** (levels - low_bits)
    low_count = 2**low_bits
    position = lax.axis_index("gx")
    left_tile = left_group
    for bit in range(low_bits):
        left_tile = pair_join(left_tile, bit, position)
    right_tile = right_group
    for bit in range(low_bits, levels):
        right_tile = pair_join(right_tile, bit, position)
    block_tile = jnp.einsum(
        "cik,cjk->cij", left_tile, right_tile, preferred_element_type=jnp.float32
    ).astype(jnp.bfloat16)
    for bit in range(low_bits):
        current = block_tile.shape[1]
        span = block_tile.shape[2]
        shaped = block_tile.reshape(group_chan, current // (2 * row_count), 2, row_count, span)
        own_bit = position // 2**bit % 2
        kept = lax.dynamic_index_in_dim(shaped, own_bit, axis=2, keepdims=False).reshape(
            group_chan, current // 2, span
        )
        sent = lax.dynamic_index_in_dim(shaped, 1 - own_bit, axis=2, keepdims=False).reshape(
            group_chan, current // 2, span
        )
        arrived = swap_with(sent, bit)
        block_tile = jnp.where(
            own_bit == 0,
            jnp.concatenate([kept, arrived], axis=2),
            jnp.concatenate([arrived, kept], axis=2),
        )
    block_tile = (
        block_tile.reshape(group_chan, row_count, low_count, high_count, row_count)
        .transpose(0, 1, 3, 2, 4)
        .reshape(group_chan, row_count, residues)
    )
    gathered = lax.all_to_all(block_tile, ("gy", "gz"), split_axis=2, concat_axis=0, tiled=True)
    update = whole_channels(gathered, out_weight, gate_value)
    return update.astype(jnp.bfloat16)


MESH = pl.DeviceIdType.MESH
LANES = 128
VMEM_ALL = 67043328
VMEM_BUDGET = 48 * 2**20


def up(value, step):
    return -(-value // step) * step


def folded(count):
    return count // LANES * LANES * 2 + LANES


def main_rows(rows):
    return rows * 8 // 10 // 16 * 16


def gate_by(gate, value):
    return (0.5 * value) * (1.0 + jnp.tanh(0.5 * gate))


def fused_kernel(
    along_y, along_z, main,
    pair_hbm, mask_hbm, proj_hbm, gate_hbm, out_w_hbm, out_ref,
    pair_ref, mask_ref, proj_ref, gate_ref, out_w_ref,
    proj_s, normed_bf, masked_bf, gate_f32, send_r, recv_r, recv_x, send_s, recv_s, send_l, recv_l,
    left_s, edge_s, edge_bf, right_s, right_bf, tri_s, send_e, recv_e, send_b, recv_b,
    load_sem, send_sem, rsem_r, rsem_x, rsem_l, rsem_b,
):
    cols, rows, chans = pair_ref.shape
    hidden = out_w_ref.shape[0]
    groups = along_y * along_z
    gc = hidden // groups
    edge = rows - main
    flat_m, flat_e = main * cols, edge * cols
    flat = flat_m + flat_e
    residues = mask_ref.shape[1]
    px, py, pz = lax.axis_index("gx"), lax.axis_index("gy"), lax.axis_index("gz")
    me = py * along_z + pz
    side = py // (along_y // 2)
    middle = along_y // 2

    def place(d):
        return (px, d // along_z, d % along_z)

    far_a = (1 - side) * (along_y - 1)
    far_b = side * (middle - 1) + (1 - side) * middle
    sibling = side * middle + (py + 1) % middle

    def to(plane, n):
        m = n if plane is py else (n + 2) % along_z
        return plane * along_z + (pz // 2 + m // 2) % (along_z // 2) * 2 + (pz + m) % 2

    partner = (1 - px, py, pz)
    barrier = pltpu.get_barrier_semaphore()

    def greet(o, carry):
        pl.semaphore_signal(barrier, inc=1, device_id=place((me + o) % groups), device_id_type=MESH)
        return carry

    with jax.named_scope("greet"):
        lax.fori_loop(1, groups, greet, 0)
        pl.semaphore_signal(barrier, inc=1, device_id=partner, device_id_type=MESH)

    loads = [
        pltpu.make_async_copy(source, target, load_sem.at[n])
        for n, (source, target) in enumerate(
            (
                (pair_hbm, pair_ref), (mask_hbm, mask_ref), (proj_hbm, proj_ref),
                (gate_hbm, gate_ref), (out_w_hbm, out_w_ref),
            )
        )
    ]
    for load in loads:
        load.start()
    with jax.named_scope("waitload"):
        loads[1].wait()
        loads[2].wait()
        proj_s[...] = proj_ref[...].astype(jnp.float32).T.astype(jnp.bfloat16)
        loads[0].wait()

    with jax.named_scope("norm"):
        mask_f = mask_ref[...].astype(jnp.float32)
        lane = lax.broadcasted_iota(jnp.int32, (rows, residues), 1)
        sub = lax.broadcasted_iota(jnp.int32, (rows, residues), 0)
        row_mask = jnp.sum(jnp.where(lane == sub + px * rows, mask_f, 0.0), axis=1, keepdims=True)
        lane_row = lax.broadcasted_iota(jnp.int32, (1, residues), 1)
        for k in range(cols):
            col_mask = jnp.sum(
                jnp.where(lane_row == me * cols + k, mask_f, 0.0), axis=1, keepdims=True
            )
            normed = layer_norm_last(pair_ref[k].astype(jnp.float32)).astype(jnp.bfloat16)
            masked = (normed.astype(jnp.float32) * (row_mask * col_mask)).astype(jnp.bfloat16)
            for target, value in ((normed_bf, normed), (masked_bf, masked)):
                target[k * main : (k + 1) * main, :] = value[0:main]
                target[flat_m + k * edge : flat_m + (k + 1) * edge, :] = value[main:rows]

    lane8 = lax.broadcasted_iota(jnp.int32, (gc, LANES), 1)
    hg = gc // 2

    def fold(value):
        count = value.shape[1]
        body, rest = count // LANES * LANES, count % LANES
        value = jnp.concatenate([value, jnp.zeros((gc, LANES - rest), jnp.float32)], axis=1)
        lower = pltpu.roll(value, hg, 0)
        tail = jnp.where(lane8 < rest, value[:, body:], pltpu.roll(lower[:, body:], rest, 1))
        return jnp.concatenate([value[:, 0:body], lower[:, 0:body], tail], axis=1)[
            0:hg
        ].astype(jnp.bfloat16)

    def unfold(value, count):
        body, rest = count // LANES * LANES, count % LANES
        tail = value[:, 2 * body : 2 * body + LANES]
        upper = jnp.concatenate([value[:, 0:body], tail], axis=1)
        lower = jnp.concatenate(
            [value[:, body : 2 * body], pltpu.roll(tail, LANES - rest, 1)], axis=1
        )
        return jnp.concatenate([upper, lower], axis=0)

    half = hidden // 2
    half_groups = groups // 2

    def gated(base, first, low, high):
        rows_of = jnp.concatenate(
            [
                proj_s[pl.ds(pl.multiple_of(base + first, half), half), :],
                proj_s[pl.ds(pl.multiple_of(base + hidden + first, half), half), :],
            ],
            axis=0,
        )
        value = lax.dot_general(
            rows_of, masked_bf[low:high, :], (((1,), (1,)), ((), ())),
            preferred_element_type=jnp.float32,
        )
        return gate_by(value[0:half], value[half:])

    def copy_r(d, slot):
        return pltpu.make_async_remote_copy(
            src_ref=send_r.at[d], dst_ref=recv_r.at[slot], send_sem=send_sem.at[0],
            recv_sem=rsem_r.at[slot], device_id=place(d), device_id_type=MESH,
        )

    def copy_rest(d, slot, count=1):
        return pltpu.make_async_remote_copy(
            src_ref=send_s.at[pl.ds(d, count)], dst_ref=recv_s.at[pl.ds(slot, count)],
            send_sem=send_sem.at[5], recv_sem=rsem_b.at[2], device_id=place(d),
            device_id_type=MESH,
        )

    def copy_x(s, n, count=1):
        return pltpu.make_async_remote_copy(
            src_ref=recv_r.at[pl.ds(s, count)], dst_ref=recv_x.at[pl.ds(s, count)],
            send_sem=send_sem.at[1], recv_sem=rsem_x.at[n],
            device_id=partner, device_id_type=MESH,
        )

    def copy_many(source, target, kind, recv_sem, d, slot, count=1):
        return pltpu.make_async_remote_copy(
            src_ref=source.at[pl.ds(d, count)], dst_ref=target.at[pl.ds(slot, count)],
            send_sem=send_sem.at[kind], recv_sem=recv_sem, device_id=place(d),
            device_id_type=MESH,
        )

    def copy_l(d, slot, n, count=1):
        return copy_many(send_l, recv_l, 2, rsem_l.at[n], d, slot, count)

    def copy_e(d, slot, count=1):
        return copy_many(send_e, recv_e, 3, rsem_b.at[0], d, slot, count)

    def copy_b(d, slot, count=1):
        return copy_many(send_b, recv_b, 4, rsem_b.at[1], d, slot, count)

    for turn in range(2):
        first = (1 - side if turn == 0 else side) * half
        with jax.named_scope(f"gated_r{turn}"):
            value = gated(2 * hidden, first, 0, flat)
            extra = gated(0, first, flat_m, flat)
            for part in range(half_groups):
                at = slice(part * gc, (part + 1) * gc)
                send_r[first // gc + part] = fold(value[at])
                send_s[first // gc + part] = fold(extra[at])
        if turn == 0:
            with jax.named_scope("barrier"):
                pl.semaphore_wait(barrier, groups)
        with jax.named_scope("start_r"):
            if turn == 0:
                order = [(plane, n) for n in range(2) for plane in (far_a, far_b)]
            else:
                order = [(py, n) for n in range(1, along_z)]
                order += [(sibling, n) for n in range(along_z)]
                order += [(plane, n) for n in range(2, along_z) for plane in (far_a, far_b)]
            for plane, n in order:
                copy_r(to(plane, n), me).start()
            if turn == 1:
                for n in range(along_z):
                    for plane in (far_a, far_b, sibling, py):
                        if n == 0 and plane is py:
                            continue
                        copy_rest(to(plane, n), me).start()
    recv_r[me] = send_r[me]
    recv_s[me] = send_s[me]
    copy_x(me, 0).start()

    for turn in range(2):
        first = (1 - side if turn == 0 else side) * half
        with jax.named_scope(f"gated_l{turn}"):
            value = gated(0, first, 0, flat_m)
            for part in range(half_groups):
                send_l[first // gc + part, :, 0:flat_m] = value[
                    part * gc : (part + 1) * gc
                ].astype(jnp.bfloat16)
    recv_l[me] = send_l[me]

    with jax.named_scope("gate"):
        loads[3].wait()
        loads[4].wait()
        gate_f32[...] = 0.5 + 0.5 * jnp.tanh(
            0.5 * jnp.dot(normed_bf[...], gate_ref[...], preferred_element_type=jnp.float32)
        )

    def lift(value, begin, width, lane):
        low, high = begin // LANES, (begin + width - 1) // LANES
        shift = (lane - begin) % LANES

        def turned(n):
            block = value[:, n * LANES : (n + 1) * LANES]
            return block if shift == 0 else pltpu.roll(block, shift, 1)

        if low == high:
            return turned(low)
        return jnp.where(lane8 < lane + high * LANES - begin, turned(low), turned(high))

    def spread_main(value, s, target):
        for k in range(cols):
            at = pl.multiple_of((s * cols + k) * gc, gc)
            target[pl.ds(at, gc), :] = lift(value, k * main, main, 0)

    def spread_right(value, s, target):
        for k in range(cols):
            at = pl.multiple_of((s * cols + k) * gc, gc)
            target[pl.ds(at, gc), :] = jnp.where(
                lane8 < main,
                lift(value, k * main, main, 0),
                lift(value, flat_m + k * edge, edge, main),
            )

    planes = (py, far_a, far_b, sibling)

    def forward(plane, n):
        s = to(plane, n)
        copy_r(s, s).wait_recv()
        copy_x(s, n).start()

    def spread_r(s):
        spread_right(unfold(recv_r[s].astype(jnp.float32), flat), s, right_s.at[px])

    def take_plane(plane, first):
        for n in range(first, along_z):
            forward(plane, n)
        for n in range(along_z):
            spread_r(to(plane, n))

    def take_far(n, carry):
        for plane in (far_a, far_b):
            forward(plane, n)
        for plane in (far_a, far_b):
            spread_r(to(plane, n))
        return carry

    def start_l(n, carry):
        for plane in (far_a, far_b, sibling, py):
            d = to(plane, n)

            @pl.when(d != me)
            def _():
                copy_l(d, me, n).start()

        return carry

    with jax.named_scope("take_own"):
        take_plane(py, 1)
    with jax.named_scope("take_far0"):
        take_far(0, 0)
    with jax.named_scope("take_sib"):
        take_plane(sibling, 0)
    with jax.named_scope("take_far1"):
        take_far(1, 0)
    with jax.named_scope("wait_send"):
        pltpu.make_async_remote_copy(
            src_ref=send_r.at[0 : groups - 1], dst_ref=recv_r.at[0 : groups - 1],
            send_sem=send_sem.at[0], recv_sem=rsem_r.at[0], device_id=partner,
            device_id_type=MESH,
        ).wait_send()
    with jax.named_scope("start_l"):
        lax.fori_loop(0, along_z, start_l, 0)
    with jax.named_scope("take_far2"):
        take_far(2, 0)
    with jax.named_scope("take_far3"):
        take_far(3, 0)

    copy_rest(0, 0, groups - 1).wait_recv()

    def take_rest(n, carry):
        for plane in planes:
            s = to(plane, n)
            value = unfold(recv_s[s].astype(jnp.float32), flat_e)
            for k in range(cols):
                at = pl.multiple_of((s * cols + k) * gc, gc)
                edge_s[pl.ds(at, gc), :] = lift(value, k * edge, edge, 0)
        return carry

    with jax.named_scope("take_rest"):
        lax.fori_loop(0, along_z, take_rest, 0, unroll=True)

    def tri(left, width, c, h, first):
        if first:
            right = right_s[h, pl.ds(c, residues, stride=gc), :].T.astype(jnp.bfloat16)
            right_bf[h, c] = right
        else:
            right = right_bf[h, c]
        block = jnp.dot(right[0:rows], left[:, 0:width], preferred_element_type=jnp.float32)
        at = pl.multiple_of(h * rows * gc, gc)
        tri_s[pl.ds(at + c, rows, stride=gc), 0:width] = block

    with jax.named_scope("tri_own"):
        for c in range(gc):
            left = edge_s[pl.ds(c, residues, stride=gc), :].astype(jnp.bfloat16)
            edge_bf[c] = left
            tri(left, edge, c, px, True)

    def take_x(n, carry):
        pltpu.make_async_remote_copy(
            src_ref=recv_r.at[0:along_y], dst_ref=recv_x.at[0:along_y],
            send_sem=send_sem.at[1], recv_sem=rsem_x.at[n], device_id=partner,
            device_id_type=MESH,
        ).wait_recv()
        for plane in planes:
            s = to(plane, n)
            spread_right(unfold(recv_x[s].astype(jnp.float32), flat), s, right_s.at[1 - px])
        return carry

    with jax.named_scope("take_x"):
        lax.fori_loop(0, along_z, take_x, 0)

    def pack(d, width):
        blocks = [None] * (up(cols * width, LANES) // LANES)
        for j in range(cols):
            at = pl.multiple_of((d * cols + j) * gc, gc)
            shift = j * width % LANES
            piece = tri_s[pl.ds(at, gc), :]
            piece = piece if shift == 0 else pltpu.roll(piece, shift, 1)
            n = j * width // LANES
            blocks[n] = piece if shift == 0 else jnp.where(lane8 < shift, blocks[n], piece)
            if shift + width > LANES:
                blocks[n + 1] = piece
        value = jnp.concatenate(blocks, axis=1)
        if width == main:
            return value.astype(jnp.bfloat16)
        return fold(value[:, 0 : cols * width])

    def ship(width, buffer, landed, copy):
        def fill(goals):
            packed = [pack(d, width) for d in goals]
            for d, value in zip(goals, packed):
                buffer[d] = value

        def begin(goals):
            for d in goals:

                @pl.when(d != me)
                def _():
                    copy(d, me).start()

        far = [to(plane, n) for n in range(along_z) for plane in (far_a, far_b)]
        near = [to(plane, n) for n in range(along_z) for plane in (sibling, py)]
        fill(far)
        begin(far)
        fill(near)
        begin(near)
        landed[me] = buffer[me]

    with jax.named_scope("tri_e"):
        for c in range(gc):
            tri(edge_bf[c], edge, c, 1 - px, True)
    with jax.named_scope("ship_e"):
        ship(edge, send_e, recv_e, copy_e)

    with jax.named_scope("take_l"):
        for n in range(along_z):
            copy_l(0, 0, n, along_y if n else along_y - 1).wait_recv()
        for n in range(along_z):
            for plane in planes:
                s = to(plane, n)
                spread_main(recv_l[s].astype(jnp.float32), s, left_s)
    with jax.named_scope("tri_m"):
        for c in range(gc):
            left = left_s[pl.ds(c, residues, stride=gc), :].astype(jnp.bfloat16)
            for h in range(2):
                tri(left, main, c, h, False)
    with jax.named_scope("ship_m"):
        ship(main, send_b, recv_b, copy_b)

    def final(received, low, width):
        count = width * cols
        if width == main:
            triangle = received[:, :, 0:count].astype(jnp.float32)
        else:
            triangle = jnp.concatenate(
                [unfold(received[s].astype(jnp.float32), count)[:, 0:count] for s in range(groups)],
                axis=0,
            )
        triangle = triangle.reshape(hidden, count)
        normed_tri = layer_norm_lead(triangle).astype(jnp.bfloat16)
        mixed = lax.dot_general(
            normed_tri, out_w_ref[...], (((0,), (0,)), ((), ())),
            preferred_element_type=jnp.float32,
        )
        first = 0 if low == 0 else flat_m
        update = (gate_f32[first : first + count] * mixed).astype(jnp.bfloat16)
        for j in range(cols):
            out_ref[j, low : low + width] = update[j * width : (j + 1) * width]

    with jax.named_scope("take_e"):
        copy_e(0, 0, groups - 1).wait_recv()
    with jax.named_scope("final_e"):
        final(recv_e, main, edge)
    with jax.named_scope("finish"):
        copy_rest(0, 0, groups - 1).wait_send()
        copy_x(0, 0, groups).wait_send()
        copy_l(0, 0, 0, groups - 1).wait_send()
        copy_e(0, 0, groups - 1).wait_send()
    with jax.named_scope("take_b"):
        copy_b(0, 0, groups - 1).wait_recv()
    with jax.named_scope("final_m"):
        final(recv_b, 0, main)
    with jax.named_scope("finish_b"):
        copy_b(0, 0, groups - 1).wait_send()


def scratch_list(main, rows, cols, chans, hidden, groups, residues):
    gc = hidden // groups
    flat_m, flat_e = main * cols, (rows - main) * cols
    flat = flat_m + flat_e
    bf, f32 = jnp.bfloat16, jnp.float32
    return [
        ((cols, rows, chans), bf),
        ((1, residues), jnp.int32),
        ((chans, 4 * hidden), bf),
        ((chans, chans), bf),
        ((hidden, chans), bf),
        ((4 * hidden, chans), bf),
        ((rows * cols, chans), bf),
        ((rows * cols, chans), bf),
        ((rows * cols, chans), f32),
        ((groups, gc // 2, folded(flat)), bf),
        ((groups, gc // 2, folded(flat)), bf),
        ((groups, gc // 2, folded(flat)), bf),
        ((groups, gc // 2, folded(flat_e)), bf),
        ((groups, gc // 2, folded(flat_e)), bf),
        ((groups, gc, up(flat_m, LANES)), bf),
        ((groups, gc, up(flat_m, LANES)), bf),
        ((residues * gc, LANES), f32),
        ((residues * gc, LANES), f32),
        ((gc, residues, LANES), bf),
        ((2, residues * gc, LANES), f32),
        ((2, gc, LANES, residues), bf),
        ((residues * gc, LANES), f32),
        ((groups, gc // 2, folded(flat_e)), bf),
        ((groups, gc // 2, folded(flat_e)), bf),
        ((groups, gc, up(flat_m, LANES)), bf),
        ((groups, gc, up(flat_m, LANES)), bf),
    ]


def fits_kernel(sizes, rows, cols, chans, hidden, residues):
    groups = sizes["gy"] * sizes["gz"]
    main = main_rows(rows)
    edge = rows - main
    if sizes["gx"] != 2 or hidden % (4 * groups) or hidden // groups != 8:
        return False
    if sizes["gy"] != 4 or sizes["gz"] != 4 or residues != 2 * rows or residues != groups * cols:
        return False
    if chans != LANES or rows > LANES or rows % 16 or main < 16 or edge < 16:
        return False
    if rows * cols % LANES * 2 > LANES or edge * cols % LANES * 2 > LANES:
        return False
    total = 0
    for shape, kind in scratch_list(main, rows, cols, chans, hidden, groups, residues):
        count = 1
        for extent in shape:
            count *= extent
        total += count * jnp.dtype(kind).itemsize
    return total < VMEM_BUDGET // 3


def local_fused(sizes, pair_map, residue_mask, proj_weight, gate_weight, out_weight):
    rows, cols, chans = pair_map.shape
    hidden = out_weight.shape[0]
    residues = residue_mask.shape[0]
    if not fits_kernel(sizes, rows, cols, chans, hidden, residues):
        return local(pair_map, residue_mask, proj_weight, gate_weight, out_weight)
    groups = sizes["gy"] * sizes["gz"]
    main = main_rows(rows)
    dma = pltpu.SemaphoreType.DMA
    vmem = pl.BlockSpec(memory_space=pltpu.VMEM)
    turned = pl.pallas_call(
        functools.partial(fused_kernel, sizes["gy"], sizes["gz"], main),
        out_shape=pltpu.VMEM((cols, rows, chans), jnp.bfloat16),
        in_specs=[pl.BlockSpec(memory_space=pltpu.HBM)] * 5,
        out_specs=vmem,
        scratch_shapes=[
            pltpu.VMEM(shape, kind)
            for shape, kind in scratch_list(main, rows, cols, chans, hidden, groups, residues)
        ]
        + [dma((5,)), dma((6,)), dma((groups,)), dma((sizes["gz"],)), dma((sizes["gz"],)), dma((3,))],
        compiler_params=pltpu.CompilerParams(
            collective_id=0, has_side_effects=True, vmem_limit_bytes=VMEM_ALL - 204800
        ),
    )(
        pair_map.transpose(1, 0, 2), residue_mask.reshape(1, residues),
        proj_weight, gate_weight, out_weight,
    )
    return turned.transpose(1, 0, 2)


def solution(mesh):
    placed = (P("gx", ("gy", "gz"), None), P(), P(), P(), P())
    return jax.shard_map(
        functools.partial(local_fused, dict(mesh.shape)), mesh=mesh, in_specs=placed, out_specs=P("gx", ("gy", "gz"), None), check_vma=False
    )
```

```python
import functools

import jax
import jax.numpy as jnp
from jax import lax
from jax.experimental import pallas as pl
from jax.experimental.pallas import tpu as pltpu
from jax.sharding import PartitionSpec as P

epsilon = 1.0


def partner_2(x, axis, bit):
    return lax.ppermute(x, axis, [(i, i ^ 1 << bit) for i in range(lax.axis_size(axis))])


def layer_norm_lead(values):
    average = jnp.mean(values, axis=0, keepdims=True)
    centred = values - average
    variance = jnp.mean(centred * centred, axis=0, keepdims=True)
    return centred * lax.rsqrt(variance + epsilon)


def layer_norm_last(values):
    average = jnp.mean(values, axis=-1, keepdims=True)
    centred = values - average
    variance = jnp.mean(centred * centred, axis=-1, keepdims=True)
    return centred * lax.rsqrt(variance + epsilon)


def swap_with(values, bit):
    return partner_2(values, "gx", bit)


def pair_join(values, bit, position):
    partner = swap_with(values, bit)
    mine_first = position // 2**bit % 2 == 0
    return jnp.where(
        mine_first,
        jnp.concatenate([values, partner], axis=1),
        jnp.concatenate([partner, values], axis=1),
    )


def whole_channels(gathered, out_weight, gate_value):
    hidden, row_count, col_count = gathered.shape
    normed_tri = layer_norm_lead(gathered.astype(jnp.float32)).astype(jnp.bfloat16)
    mixed_out = lax.dot_general(
        normed_tri.reshape(hidden, row_count * col_count),
        out_weight,
        (((0,), (0,)), ((), ())),
        preferred_element_type=jnp.float32,
    )
    return gate_value * mixed_out.reshape(row_count, col_count, out_weight.shape[1])


def local(pair_map, residue_mask, proj_weight, gate_weight, out_weight):
    row_count, col_count, chan_count = pair_map.shape
    hidden = out_weight.shape[0]
    residues = residue_mask.shape[0]
    along_x = lax.axis_size("gx")
    along_y = lax.axis_size("gy")
    along_z = lax.axis_size("gz")
    mask_float = residue_mask.astype(jnp.float32)
    row_mask = lax.dynamic_slice_in_dim(mask_float, lax.axis_index("gx") * row_count, row_count)
    col_mask = lax.dynamic_slice_in_dim(
        mask_float, (lax.axis_index("gy") * along_z + lax.axis_index("gz")) * col_count, col_count
    )
    normed = layer_norm_last(pair_map.astype(jnp.float32)).astype(jnp.bfloat16)
    flattened = normed.reshape(row_count * col_count, chan_count)
    projected = lax.dot_general(
        proj_weight, flattened, (((0,), (1,)), ((), ())), preferred_element_type=jnp.float32
    ).reshape(4 * hidden, row_count, col_count)
    pair_mask = (row_mask[:, None] * col_mask[None, :])[None, :, :]
    left_proj = (
        jax.nn.sigmoid(projected[:hidden]) * projected[hidden : 2 * hidden] * pair_mask
    ).astype(jnp.bfloat16)
    right_proj = (
        jax.nn.sigmoid(projected[2 * hidden : 3 * hidden]) * projected[3 * hidden :] * pair_mask
    ).astype(jnp.bfloat16)
    gate_value = jax.nn.sigmoid(
        jnp.dot(flattened, gate_weight, preferred_element_type=jnp.float32)
    ).reshape(row_count, col_count, chan_count)
    group_count = along_y * along_z
    group_chan = hidden // group_count
    left_group, right_group = (
        lax.all_to_all(left_proj, ("gy", "gz"), split_axis=0, concat_axis=2, tiled=True),
        lax.all_to_all(right_proj, ("gy", "gz"), split_axis=0, concat_axis=2, tiled=True),
    )
    levels = along_x.bit_length() - 1
    low_bits = levels // 2
    high_count = 2 ** (levels - low_bits)
    low_count = 2**low_bits
    position = lax.axis_index("gx")
    left_tile = left_group
    for bit in range(low_bits):
        left_tile = pair_join(left_tile, bit, position)
    right_tile = right_group
    for bit in range(low_bits, levels):
        right_tile = pair_join(right_tile, bit, position)
    block_tile = jnp.einsum(
        "cik,cjk->cij", left_tile, right_tile, preferred_element_type=jnp.float32
    ).astype(jnp.bfloat16)
    for bit in range(low_bits):
        current = block_tile.shape[1]
        span = block_tile.shape[2]
        shaped = block_tile.reshape(group_chan, current // (2 * row_count), 2, row_count, span)
        own_bit = position // 2**bit % 2
        kept = lax.dynamic_index_in_dim(shaped, own_bit, axis=2, keepdims=False).reshape(
            group_chan, current // 2, span
        )
        sent = lax.dynamic_index_in_dim(shaped, 1 - own_bit, axis=2, keepdims=False).reshape(
            group_chan, current // 2, span
        )
        arrived = swap_with(sent, bit)
        block_tile = jnp.where(
            own_bit == 0,
            jnp.concatenate([kept, arrived], axis=2),
            jnp.concatenate([arrived, kept], axis=2),
        )
    block_tile = (
        block_tile.reshape(group_chan, row_count, low_count, high_count, row_count)
        .transpose(0, 1, 3, 2, 4)
        .reshape(group_chan, row_count, residues)
    )
    gathered = lax.all_to_all(block_tile, ("gy", "gz"), split_axis=2, concat_axis=0, tiled=True)
    update = whole_channels(gathered, out_weight, gate_value)
    return update.astype(jnp.bfloat16)


MESH = pl.DeviceIdType.MESH
LANES = 128
VMEM_ALL = 67043328
VMEM_BUDGET = 48 * 2**20


def up(value, step):
    return -(-value // step) * step


def folded(count):
    return count // LANES * LANES * 2 + LANES


def main_rows(rows):
    return rows * 8 // 10 // 16 * 16


def gate_by(gate, value):
    return (0.5 * value) * (1.0 + jnp.tanh(0.5 * gate))


def fused_kernel(
    along_y, along_z, main,
    pair_hbm, mask_hbm, proj_hbm, gate_hbm, out_w_hbm, out_ref,
    pair_ref, mask_ref, proj_ref, gate_ref, out_w_ref,
    proj_s, normed_bf, masked_bf, gate_f32, send_r, recv_r, recv_x, send_s, recv_s, send_l, recv_l,
    left_s, edge_s, edge_bf, right_s, right_bf, tri_s, send_e, recv_e, send_b, recv_b,
    load_sem, send_sem, rsem_r, rsem_x, rsem_l, rsem_b,
):
    cols, rows, chans = pair_ref.shape
    hidden = out_w_ref.shape[0]
    groups = along_y * along_z
    gc = hidden // groups
    edge = rows - main
    flat_m, flat_e = main * cols, edge * cols
    flat = flat_m + flat_e
    residues = mask_ref.shape[1]
    px, py, pz = lax.axis_index("gx"), lax.axis_index("gy"), lax.axis_index("gz")
    me = py * along_z + pz
    side = py // (along_y // 2)
    middle = along_y // 2

    def place(d):
        return (px, d // along_z, d % along_z)

    far_a = (1 - side) * (along_y - 1)
    far_b = side * (middle - 1) + (1 - side) * middle
    sibling = side * middle + (py + 1) % middle

    def to(plane, n):
        m = n if plane is py else (n + 2) % along_z
        return plane * along_z + (pz // 2 + m // 2) % (along_z // 2) * 2 + (pz + m) % 2

    partner = (1 - px, py, pz)
    barrier = pltpu.get_barrier_semaphore()

    def greet(o, carry):
        pl.semaphore_signal(barrier, inc=1, device_id=place((me + o) % groups), device_id_type=MESH)
        return carry

    with jax.named_scope("greet"):
        lax.fori_loop(1, groups, greet, 0)
        pl.semaphore_signal(barrier, inc=1, device_id=partner, device_id_type=MESH)

    loads = [
        pltpu.make_async_copy(source, target, load_sem.at[n])
        for n, (source, target) in enumerate(
            (
                (pair_hbm, pair_ref), (mask_hbm, mask_ref), (proj_hbm, proj_ref),
                (gate_hbm, gate_ref), (out_w_hbm, out_w_ref),
            )
        )
    ]
    for load in loads:
        load.start()
    with jax.named_scope("waitload"):
        loads[1].wait()
        loads[2].wait()
        proj_s[...] = proj_ref[...].astype(jnp.float32).T.astype(jnp.bfloat16)
        loads[0].wait()

    with jax.named_scope("norm"):
        mask_f = mask_ref[...].astype(jnp.float32)
        lane = lax.broadcasted_iota(jnp.int32, (rows, residues), 1)
        sub = lax.broadcasted_iota(jnp.int32, (rows, residues), 0)
        row_mask = jnp.sum(jnp.where(lane == sub + px * rows, mask_f, 0.0), axis=1, keepdims=True)
        lane_row = lax.broadcasted_iota(jnp.int32, (1, residues), 1)
        for k in range(cols):
            col_mask = jnp.sum(
                jnp.where(lane_row == me * cols + k, mask_f, 0.0), axis=1, keepdims=True
            )
            normed = layer_norm_last(pair_ref[k].astype(jnp.float32)).astype(jnp.bfloat16)
            masked = (normed.astype(jnp.float32) * (row_mask * col_mask)).astype(jnp.bfloat16)
            for target, value in ((normed_bf, normed), (masked_bf, masked)):
                target[k * main : (k + 1) * main, :] = value[0:main]
                target[flat_m + k * edge : flat_m + (k + 1) * edge, :] = value[main:rows]

    lane8 = lax.broadcasted_iota(jnp.int32, (gc, LANES), 1)
    hg = gc // 2

    def fold(value):
        count = value.shape[1]
        body, rest = count // LANES * LANES, count % LANES
        value = jnp.concatenate([value, jnp.zeros((gc, LANES - rest), jnp.float32)], axis=1)
        lower = pltpu.roll(value, hg, 0)
        tail = jnp.where(lane8 < rest, value[:, body:], pltpu.roll(lower[:, body:], rest, 1))
        return jnp.concatenate([value[:, 0:body], lower[:, 0:body], tail], axis=1)[
            0:hg
        ].astype(jnp.bfloat16)

    def unfold(value, count):
        body, rest = count // LANES * LANES, count % LANES
        tail = value[:, 2 * body : 2 * body + LANES]
        upper = jnp.concatenate([value[:, 0:body], tail], axis=1)
        lower = jnp.concatenate(
            [value[:, body : 2 * body], pltpu.roll(tail, LANES - rest, 1)], axis=1
        )
        return jnp.concatenate([upper, lower], axis=0)

    half = hidden // 2
    half_groups = groups // 2

    def gated(base, first, low, high):
        rows_of = jnp.concatenate(
            [
                proj_s[pl.ds(pl.multiple_of(base + first, half), half), :],
                proj_s[pl.ds(pl.multiple_of(base + hidden + first, half), half), :],
            ],
            axis=0,
        )
        value = lax.dot_general(
            rows_of, masked_bf[low:high, :], (((1,), (1,)), ((), ())),
            preferred_element_type=jnp.float32,
        )
        return gate_by(value[0:half], value[half:])

    def copy_r(d, slot):
        return pltpu.make_async_remote_copy(
            src_ref=send_r.at[d], dst_ref=recv_r.at[slot], send_sem=send_sem.at[0],
            recv_sem=rsem_r.at[slot], device_id=place(d), device_id_type=MESH,
        )

    def copy_rest(d, slot, count=1):
        return pltpu.make_async_remote_copy(
            src_ref=send_s.at[pl.ds(d, count)], dst_ref=recv_s.at[pl.ds(slot, count)],
            send_sem=send_sem.at[5], recv_sem=rsem_b.at[2], device_id=place(d),
            device_id_type=MESH,
        )

    def copy_x(s, n, count=1):
        return pltpu.make_async_remote_copy(
            src_ref=recv_r.at[pl.ds(s, count)], dst_ref=recv_x.at[pl.ds(s, count)],
            send_sem=send_sem.at[1], recv_sem=rsem_x.at[n],
            device_id=partner, device_id_type=MESH,
        )

    def copy_many(source, target, kind, recv_sem, d, slot, count=1):
        return pltpu.make_async_remote_copy(
            src_ref=source.at[pl.ds(d, count)], dst_ref=target.at[pl.ds(slot, count)],
            send_sem=send_sem.at[kind], recv_sem=recv_sem, device_id=place(d),
            device_id_type=MESH,
        )

    def copy_l(d, slot, n, count=1):
        return copy_many(send_l, recv_l, 2, rsem_l.at[n], d, slot, count)

    def copy_e(d, slot, count=1):
        return copy_many(send_e, recv_e, 3, rsem_b.at[0], d, slot, count)

    def copy_b(d, slot, count=1):
        return copy_many(send_b, recv_b, 4, rsem_b.at[1], d, slot, count)

    for turn in range(2):
        first = (1 - side if turn == 0 else side) * half
        with jax.named_scope(f"gated_r{turn}"):
            value = gated(2 * hidden, first, 0, flat)
            extra = gated(0, first, flat_m, flat)
            for part in range(half_groups):
                at = slice(part * gc, (part + 1) * gc)
                send_r[first // gc + part] = fold(value[at])
                send_s[first // gc + part] = fold(extra[at])
        if turn == 0:
            with jax.named_scope("barrier"):
                pl.semaphore_wait(barrier, groups)
        with jax.named_scope("start_r"):
            if turn == 0:
                order = [(plane, n) for n in range(2) for plane in (far_a, far_b)]
            else:
                order = [(sibling, n) for n in range(along_z)]
                order += [(py, n) for n in range(1, along_z)]
                order += [(plane, n) for n in range(2, along_z) for plane in (far_a, far_b)]
            for plane, n in order:
                copy_r(to(plane, n), me).start()
            if turn == 1:
                for n in range(along_z):
                    for plane in (far_a, far_b, sibling, py):
                        if n == 0 and plane is py:
                            continue
                        copy_rest(to(plane, n), me).start()
    recv_r[me] = send_r[me]
    recv_s[me] = send_s[me]
    copy_x(me, 0).start()

    for turn in range(2):
        first = (1 - side if turn == 0 else side) * half
        with jax.named_scope(f"gated_l{turn}"):
            value = gated(0, first, 0, flat_m)
            for part in range(half_groups):
                send_l[first // gc + part, :, 0:flat_m] = value[
                    part * gc : (part + 1) * gc
                ].astype(jnp.bfloat16)
    recv_l[me] = send_l[me]

    with jax.named_scope("gate"):
        loads[3].wait()
        loads[4].wait()
        gate_f32[...] = 0.5 + 0.5 * jnp.tanh(
            0.5 * jnp.dot(normed_bf[...], gate_ref[...], preferred_element_type=jnp.float32)
        )

    def lift(value, begin, width, lane):
        low, high = begin // LANES, (begin + width - 1) // LANES
        shift = (lane - begin) % LANES

        def turned(n):
            block = value[:, n * LANES : (n + 1) * LANES]
            return block if shift == 0 else pltpu.roll(block, shift, 1)

        if low == high:
            return turned(low)
        return jnp.where(lane8 < lane + high * LANES - begin, turned(low), turned(high))

    def spread_main(value, s, target):
        for k in range(cols):
            at = pl.multiple_of((s * cols + k) * gc, gc)
            target[pl.ds(at, gc), :] = lift(value, k * main, main, 0)

    def spread_right(value, s, target):
        for k in range(cols):
            at = pl.multiple_of((s * cols + k) * gc, gc)
            target[pl.ds(at, gc), :] = jnp.where(
                lane8 < main,
                lift(value, k * main, main, 0),
                lift(value, flat_m + k * edge, edge, main),
            )

    planes = (py, far_a, far_b, sibling)

    def forward(plane, n):
        s = to(plane, n)
        copy_r(s, s).wait_recv()
        copy_x(s, n).start()

    def spread_r(s):
        spread_right(unfold(recv_r[s].astype(jnp.float32), flat), s, right_s.at[px])

    def take_plane(plane, first):
        for n in range(first, along_z):
            forward(plane, n)
        for n in range(along_z):
            spread_r(to(plane, n))

    def take_far(n, carry):
        for plane in (far_a, far_b):
            forward(plane, n)
        for plane in (far_a, far_b):
            spread_r(to(plane, n))
        return carry

    def start_l():
        for plane in (far_a, far_b, sibling, py):
            for n in range(0 if plane is not py else 1, along_z):
                copy_l(to(plane, n), me, n).start()

    with jax.named_scope("take_own"):
        take_plane(py, 1)
    with jax.named_scope("take_far0"):
        take_far(0, 0)
    with jax.named_scope("take_sib"):
        take_plane(sibling, 0)
    with jax.named_scope("take_far1"):
        take_far(1, 0)
    with jax.named_scope("wait_send"):
        pltpu.make_async_remote_copy(
            src_ref=send_r.at[0 : groups - 1], dst_ref=recv_r.at[0 : groups - 1],
            send_sem=send_sem.at[0], recv_sem=rsem_r.at[0], device_id=partner,
            device_id_type=MESH,
        ).wait_send()
    with jax.named_scope("start_l"):
        start_l()
    with jax.named_scope("take_far2"):
        take_far(2, 0)
    with jax.named_scope("take_far3"):
        take_far(3, 0)

    copy_rest(0, 0, groups - 1).wait_recv()

    def take_rest(n, carry):
        for plane in planes:
            s = to(plane, n)
            value = unfold(recv_s[s].astype(jnp.float32), flat_e)
            for k in range(cols):
                at = pl.multiple_of((s * cols + k) * gc, gc)
                edge_s[pl.ds(at, gc), :] = lift(value, k * edge, edge, 0)
        return carry

    with jax.named_scope("take_rest"):
        lax.fori_loop(0, along_z, take_rest, 0, unroll=True)

    def tri(left, width, c, h, first):
        if first:
            right = right_s[h, pl.ds(c, residues, stride=gc), :].T.astype(jnp.bfloat16)
            right_bf[h, c] = right
        else:
            right = right_bf[h, c]
        block = jnp.dot(right[0:rows], left[:, 0:width], preferred_element_type=jnp.float32)
        at = pl.multiple_of(h * rows * gc, gc)
        tri_s[pl.ds(at + c, rows, stride=gc), 0:width] = block

    with jax.named_scope("tri_own"):
        for c in range(gc):
            left = edge_s[pl.ds(c, residues, stride=gc), :].astype(jnp.bfloat16)
            edge_bf[c] = left
            tri(left, edge, c, px, True)

    def take_x(n, carry):
        pltpu.make_async_remote_copy(
            src_ref=recv_r.at[0:along_y], dst_ref=recv_x.at[0:along_y],
            send_sem=send_sem.at[1], recv_sem=rsem_x.at[n], device_id=partner,
            device_id_type=MESH,
        ).wait_recv()
        for plane in planes:
            s = to(plane, n)
            spread_right(unfold(recv_x[s].astype(jnp.float32), flat), s, right_s.at[1 - px])
        return carry

    with jax.named_scope("take_x"):
        lax.fori_loop(0, along_z, take_x, 0)

    def pack(d, width):
        blocks = [None] * (up(cols * width, LANES) // LANES)
        for j in range(cols):
            at = pl.multiple_of((d * cols + j) * gc, gc)
            shift = j * width % LANES
            piece = tri_s[pl.ds(at, gc), :]
            piece = piece if shift == 0 else pltpu.roll(piece, shift, 1)
            n = j * width // LANES
            blocks[n] = piece if shift == 0 else jnp.where(lane8 < shift, blocks[n], piece)
            if shift + width > LANES:
                blocks[n + 1] = piece
        value = jnp.concatenate(blocks, axis=1)
        if width == main:
            return value.astype(jnp.bfloat16)
        return fold(value[:, 0 : cols * width])

    def ship(width, buffer, landed, copy):
        def fill(goals):
            packed = [pack(d, width) for d in goals]
            for d, value in zip(goals, packed):
                buffer[d] = value

        def begin(goals):
            for d in goals:

                @pl.when(d != me)
                def _():
                    copy(d, me).start()

        far = [to(plane, n) for plane in (far_a, far_b) for n in range(along_z)]
        near = [to(plane, n) for n in range(along_z) for plane in (sibling, py)]
        fill(far)
        begin(far)
        fill(near)
        begin(near)
        landed[me] = buffer[me]

    with jax.named_scope("tri_e"):
        for c in range(gc):
            tri(edge_bf[c], edge, c, 1 - px, True)
    with jax.named_scope("ship_e"):
        ship(edge, send_e, recv_e, copy_e)

    with jax.named_scope("take_l"):
        for n in range(along_z):
            copy_l(0, 0, n, along_y if n else along_y - 1).wait_recv()
        for n in range(along_z):
            for plane in planes:
                s = to(plane, n)
                spread_main(recv_l[s].astype(jnp.float32), s, left_s)
    with jax.named_scope("tri_m"):
        for c in range(gc):
            left = left_s[pl.ds(c, residues, stride=gc), :].astype(jnp.bfloat16)
            for h in range(2):
                tri(left, main, c, h, False)
    with jax.named_scope("ship_m"):
        ship(main, send_b, recv_b, copy_b)

    def final(received, low, width):
        count = width * cols
        if width == main:
            triangle = received[:, :, 0:count].astype(jnp.float32)
        else:
            triangle = jnp.concatenate(
                [unfold(received[s].astype(jnp.float32), count)[:, 0:count] for s in range(groups)],
                axis=0,
            )
        triangle = triangle.reshape(hidden, count)
        normed_tri = layer_norm_lead(triangle).astype(jnp.bfloat16)
        mixed = lax.dot_general(
            normed_tri, out_w_ref[...], (((0,), (0,)), ((), ())),
            preferred_element_type=jnp.float32,
        )
        first = 0 if low == 0 else flat_m
        update = (gate_f32[first : first + count] * mixed).astype(jnp.bfloat16)
        for j in range(cols):
            out_ref[j, low : low + width] = update[j * width : (j + 1) * width]

    with jax.named_scope("take_e"):
        copy_e(0, 0, groups - 1).wait_recv()
    with jax.named_scope("final_e"):
        final(recv_e, main, edge)
    with jax.named_scope("finish"):
        copy_rest(0, 0, groups - 1).wait_send()
        copy_x(0, 0, groups).wait_send()
        copy_l(0, 0, 0, groups - 1).wait_send()
        copy_e(0, 0, groups - 1).wait_send()
    with jax.named_scope("take_b"):
        copy_b(0, 0, groups - 1).wait_recv()
    with jax.named_scope("final_m"):
        final(recv_b, 0, main)
    with jax.named_scope("finish_b"):
        copy_b(0, 0, groups - 1).wait_send()


def scratch_list(main, rows, cols, chans, hidden, groups, residues):
    gc = hidden // groups
    flat_m, flat_e = main * cols, (rows - main) * cols
    flat = flat_m + flat_e
    bf, f32 = jnp.bfloat16, jnp.float32
    return [
        ((cols, rows, chans), bf),
        ((1, residues), jnp.int32),
        ((chans, 4 * hidden), bf),
        ((chans, chans), bf),
        ((hidden, chans), bf),
        ((4 * hidden, chans), bf),
        ((rows * cols, chans), bf),
        ((rows * cols, chans), bf),
        ((rows * cols, chans), f32),
        ((groups, gc // 2, folded(flat)), bf),
        ((groups, gc // 2, folded(flat)), bf),
        ((groups, gc // 2, folded(flat)), bf),
        ((groups, gc // 2, folded(flat_e)), bf),
        ((groups, gc // 2, folded(flat_e)), bf),
        ((groups, gc, up(flat_m, LANES)), bf),
        ((groups, gc, up(flat_m, LANES)), bf),
        ((residues * gc, LANES), f32),
        ((residues * gc, LANES), f32),
        ((gc, residues, LANES), bf),
        ((2, residues * gc, LANES), f32),
        ((2, gc, LANES, residues), bf),
        ((residues * gc, LANES), f32),
        ((groups, gc // 2, folded(flat_e)), bf),
        ((groups, gc // 2, folded(flat_e)), bf),
        ((groups, gc, up(flat_m, LANES)), bf),
        ((groups, gc, up(flat_m, LANES)), bf),
    ]


def fits_kernel(sizes, rows, cols, chans, hidden, residues):
    groups = sizes["gy"] * sizes["gz"]
    main = main_rows(rows)
    edge = rows - main
    if sizes["gx"] != 2 or hidden % (4 * groups) or hidden // groups != 8:
        return False
    if sizes["gy"] != 4 or sizes["gz"] != 4 or residues != 2 * rows or residues != groups * cols:
        return False
    if chans != LANES or rows > LANES or rows % 16 or main < 16 or edge < 16:
        return False
    if rows * cols % LANES * 2 > LANES or edge * cols % LANES * 2 > LANES:
        return False
    total = 0
    for shape, kind in scratch_list(main, rows, cols, chans, hidden, groups, residues):
        count = 1
        for extent in shape:
            count *= extent
        total += count * jnp.dtype(kind).itemsize
    return total < VMEM_BUDGET // 3


def local_fused(sizes, pair_map, residue_mask, proj_weight, gate_weight, out_weight):
    rows, cols, chans = pair_map.shape
    hidden = out_weight.shape[0]
    residues = residue_mask.shape[0]
    if not fits_kernel(sizes, rows, cols, chans, hidden, residues):
        return local(pair_map, residue_mask, proj_weight, gate_weight, out_weight)
    groups = sizes["gy"] * sizes["gz"]
    main = main_rows(rows)
    dma = pltpu.SemaphoreType.DMA
    vmem = pl.BlockSpec(memory_space=pltpu.VMEM)
    turned = pl.pallas_call(
        functools.partial(fused_kernel, sizes["gy"], sizes["gz"], main),
        out_shape=pltpu.VMEM((cols, rows, chans), jnp.bfloat16),
        in_specs=[pl.BlockSpec(memory_space=pltpu.HBM)] * 5,
        out_specs=vmem,
        scratch_shapes=[
            pltpu.VMEM(shape, kind)
            for shape, kind in scratch_list(main, rows, cols, chans, hidden, groups, residues)
        ]
        + [dma((5,)), dma((6,)), dma((groups,)), dma((sizes["gz"],)), dma((sizes["gz"],)), dma((3,))],
        compiler_params=pltpu.CompilerParams(
            collective_id=0, has_side_effects=True, vmem_limit_bytes=VMEM_ALL - 204800
        ),
    )(
        pair_map.transpose(1, 0, 2), residue_mask.reshape(1, residues),
        proj_weight, gate_weight, out_weight,
    )
    return turned.transpose(1, 0, 2)


def solution(mesh):
    placed = (P("gx", ("gy", "gz"), None), P(), P(), P(), P())
    return jax.shard_map(
        functools.partial(local_fused, dict(mesh.shape)), mesh=mesh, in_specs=placed, out_specs=P("gx", ("gy", "gz"), None), check_vma=False
    )
```

```python
import functools

import jax
import jax.numpy as jnp
from jax import lax
from jax.experimental import pallas as pl
from jax.experimental.pallas import tpu as pltpu
from jax.sharding import PartitionSpec as P

epsilon = 1.0


def partner_2(x, axis, bit):
    return lax.ppermute(x, axis, [(i, i ^ 1 << bit) for i in range(lax.axis_size(axis))])


def layer_norm_lead(values):
    average = jnp.mean(values, axis=0, keepdims=True)
    centred = values - average
    variance = jnp.mean(centred * centred, axis=0, keepdims=True)
    return centred * lax.rsqrt(variance + epsilon)


def layer_norm_last(values):
    average = jnp.mean(values, axis=-1, keepdims=True)
    centred = values - average
    variance = jnp.mean(centred * centred, axis=-1, keepdims=True)
    return centred * lax.rsqrt(variance + epsilon)


def swap_with(values, bit):
    return partner_2(values, "gx", bit)


def pair_join(values, bit, position):
    partner = swap_with(values, bit)
    mine_first = position // 2**bit % 2 == 0
    return jnp.where(
        mine_first,
        jnp.concatenate([values, partner], axis=1),
        jnp.concatenate([partner, values], axis=1),
    )


def whole_channels(gathered, out_weight, gate_value):
    hidden, row_count, col_count = gathered.shape
    normed_tri = layer_norm_lead(gathered.astype(jnp.float32)).astype(jnp.bfloat16)
    mixed_out = lax.dot_general(
        normed_tri.reshape(hidden, row_count * col_count),
        out_weight,
        (((0,), (0,)), ((), ())),
        preferred_element_type=jnp.float32,
    )
    return gate_value * mixed_out.reshape(row_count, col_count, out_weight.shape[1])


def local(pair_map, residue_mask, proj_weight, gate_weight, out_weight):
    row_count, col_count, chan_count = pair_map.shape
    hidden = out_weight.shape[0]
    residues = residue_mask.shape[0]
    along_x = lax.axis_size("gx")
    along_y = lax.axis_size("gy")
    along_z = lax.axis_size("gz")
    mask_float = residue_mask.astype(jnp.float32)
    row_mask = lax.dynamic_slice_in_dim(mask_float, lax.axis_index("gx") * row_count, row_count)
    col_mask = lax.dynamic_slice_in_dim(
        mask_float, (lax.axis_index("gy") * along_z + lax.axis_index("gz")) * col_count, col_count
    )
    normed = layer_norm_last(pair_map.astype(jnp.float32)).astype(jnp.bfloat16)
    flattened = normed.reshape(row_count * col_count, chan_count)
    projected = lax.dot_general(
        proj_weight, flattened, (((0,), (1,)), ((), ())), preferred_element_type=jnp.float32
    ).reshape(4 * hidden, row_count, col_count)
    pair_mask = (row_mask[:, None] * col_mask[None, :])[None, :, :]
    left_proj = (
        jax.nn.sigmoid(projected[:hidden]) * projected[hidden : 2 * hidden] * pair_mask
    ).astype(jnp.bfloat16)
    right_proj = (
        jax.nn.sigmoid(projected[2 * hidden : 3 * hidden]) * projected[3 * hidden :] * pair_mask
    ).astype(jnp.bfloat16)
    gate_value = jax.nn.sigmoid(
        jnp.dot(flattened, gate_weight, preferred_element_type=jnp.float32)
    ).reshape(row_count, col_count, chan_count)
    group_count = along_y * along_z
    group_chan = hidden // group_count
    left_group, right_group = (
        lax.all_to_all(left_proj, ("gy", "gz"), split_axis=0, concat_axis=2, tiled=True),
        lax.all_to_all(right_proj, ("gy", "gz"), split_axis=0, concat_axis=2, tiled=True),
    )
    levels = along_x.bit_length() - 1
    low_bits = levels // 2
    high_count = 2 ** (levels - low_bits)
    low_count = 2**low_bits
    position = lax.axis_index("gx")
    left_tile = left_group
    for bit in range(low_bits):
        left_tile = pair_join(left_tile, bit, position)
    right_tile = right_group
    for bit in range(low_bits, levels):
        right_tile = pair_join(right_tile, bit, position)
    block_tile = jnp.einsum(
        "cik,cjk->cij", left_tile, right_tile, preferred_element_type=jnp.float32
    ).astype(jnp.bfloat16)
    for bit in range(low_bits):
        current = block_tile.shape[1]
        span = block_tile.shape[2]
        shaped = block_tile.reshape(group_chan, current // (2 * row_count), 2, row_count, span)
        own_bit = position // 2**bit % 2
        kept = lax.dynamic_index_in_dim(shaped, own_bit, axis=2, keepdims=False).reshape(
            group_chan, current // 2, span
        )
        sent = lax.dynamic_index_in_dim(shaped, 1 - own_bit, axis=2, keepdims=False).reshape(
            group_chan, current // 2, span
        )
        arrived = swap_with(sent, bit)
        block_tile = jnp.where(
            own_bit == 0,
            jnp.concatenate([kept, arrived], axis=2),
            jnp.concatenate([arrived, kept], axis=2),
        )
    block_tile = (
        block_tile.reshape(group_chan, row_count, low_count, high_count, row_count)
        .transpose(0, 1, 3, 2, 4)
        .reshape(group_chan, row_count, residues)
    )
    gathered = lax.all_to_all(block_tile, ("gy", "gz"), split_axis=2, concat_axis=0, tiled=True)
    update = whole_channels(gathered, out_weight, gate_value)
    return update.astype(jnp.bfloat16)


MESH = pl.DeviceIdType.MESH
LANES = 128
VMEM_ALL = 67043328
VMEM_BUDGET = 48 * 2**20


def up(value, step):
    return -(-value // step) * step


def folded(count):
    return count // LANES * LANES * 2 + LANES


def main_rows(rows):
    return rows * 8 // 10 // 16 * 16


def gate_by(gate, value):
    return (0.5 * value) * (1.0 + jnp.tanh(0.5 * gate))


def fused_kernel(
    along_y, along_z, main,
    pair_hbm, mask_hbm, proj_hbm, gate_hbm, out_w_hbm, out_ref,
    pair_ref, mask_ref, proj_ref, gate_ref, out_w_ref,
    proj_s, normed_bf, masked_bf, gate_f32, send_r, recv_r, recv_x, send_s, recv_s, send_l, recv_l,
    left_s, edge_s, edge_bf, right_s, right_bf, tri_s, send_e, recv_e, send_b, recv_b,
    load_sem, send_sem, rsem_r, rsem_x, rsem_l, rsem_b,
):
    cols, rows, chans = pair_ref.shape
    hidden = out_w_ref.shape[0]
    groups = along_y * along_z
    gc = hidden // groups
    edge = rows - main
    flat_m, flat_e = main * cols, edge * cols
    flat = flat_m + flat_e
    residues = mask_ref.shape[1]
    px, py, pz = lax.axis_index("gx"), lax.axis_index("gy"), lax.axis_index("gz")
    me = py * along_z + pz
    side = py // (along_y // 2)
    middle = along_y // 2

    def place(d):
        return (px, d // along_z, d % along_z)

    far_a = (1 - side) * (along_y - 1)
    far_b = side * (middle - 1) + (1 - side) * middle
    sibling = side * middle + (py + 1) % middle

    def to(plane, n):
        m = n if plane is py else (n + 2) % along_z
        return plane * along_z + (pz // 2 + m // 2) % (along_z // 2) * 2 + (pz + m) % 2

    partner = (1 - px, py, pz)
    barrier = pltpu.get_barrier_semaphore()

    def greet(o, carry):
        pl.semaphore_signal(barrier, inc=1, device_id=place((me + o) % groups), device_id_type=MESH)
        return carry

    with jax.named_scope("greet"):
        lax.fori_loop(1, groups, greet, 0)
        pl.semaphore_signal(barrier, inc=1, device_id=partner, device_id_type=MESH)

    loads = [
        pltpu.make_async_copy(source, target, load_sem.at[n])
        for n, (source, target) in enumerate(
            (
                (pair_hbm, pair_ref), (mask_hbm, mask_ref), (proj_hbm, proj_ref),
                (gate_hbm, gate_ref), (out_w_hbm, out_w_ref),
            )
        )
    ]
    for load in loads:
        load.start()
    with jax.named_scope("waitload"):
        loads[1].wait()
        loads[2].wait()
        proj_s[...] = proj_ref[...].astype(jnp.float32).T.astype(jnp.bfloat16)
        loads[0].wait()

    with jax.named_scope("norm"):
        mask_f = mask_ref[...].astype(jnp.float32)
        lane = lax.broadcasted_iota(jnp.int32, (rows, residues), 1)
        sub = lax.broadcasted_iota(jnp.int32, (rows, residues), 0)
        row_mask = jnp.sum(jnp.where(lane == sub + px * rows, mask_f, 0.0), axis=1, keepdims=True)
        lane_row = lax.broadcasted_iota(jnp.int32, (1, residues), 1)
        for k in range(cols):
            col_mask = jnp.sum(
                jnp.where(lane_row == me * cols + k, mask_f, 0.0), axis=1, keepdims=True
            )
            normed = layer_norm_last(pair_ref[k].astype(jnp.float32)).astype(jnp.bfloat16)
            masked = (normed.astype(jnp.float32) * (row_mask * col_mask)).astype(jnp.bfloat16)
            for target, value in ((normed_bf, normed), (masked_bf, masked)):
                target[k * main : (k + 1) * main, :] = value[0:main]
                target[flat_m + k * edge : flat_m + (k + 1) * edge, :] = value[main:rows]

    lane8 = lax.broadcasted_iota(jnp.int32, (gc, LANES), 1)
    hg = gc // 2

    def fold(value):
        count = value.shape[1]
        body, rest = count // LANES * LANES, count % LANES
        value = jnp.concatenate([value, jnp.zeros((gc, LANES - rest), jnp.float32)], axis=1)
        lower = pltpu.roll(value, hg, 0)
        tail = jnp.where(lane8 < rest, value[:, body:], pltpu.roll(lower[:, body:], rest, 1))
        return jnp.concatenate([value[:, 0:body], lower[:, 0:body], tail], axis=1)[
            0:hg
        ].astype(jnp.bfloat16)

    def unfold(value, count):
        body, rest = count // LANES * LANES, count % LANES
        tail = value[:, 2 * body : 2 * body + LANES]
        upper = jnp.concatenate([value[:, 0:body], tail], axis=1)
        lower = jnp.concatenate(
            [value[:, body : 2 * body], pltpu.roll(tail, LANES - rest, 1)], axis=1
        )
        return jnp.concatenate([upper, lower], axis=0)

    half = hidden // 2
    half_groups = groups // 2

    def gated(base, first, low, high):
        rows_of = jnp.concatenate(
            [
                proj_s[pl.ds(pl.multiple_of(base + first, half), half), :],
                proj_s[pl.ds(pl.multiple_of(base + hidden + first, half), half), :],
            ],
            axis=0,
        )
        value = lax.dot_general(
            rows_of, masked_bf[low:high, :], (((1,), (1,)), ((), ())),
            preferred_element_type=jnp.float32,
        )
        return gate_by(value[0:half], value[half:])

    def copy_r(d, slot):
        return pltpu.make_async_remote_copy(
            src_ref=send_r.at[d], dst_ref=recv_r.at[slot], send_sem=send_sem.at[0],
            recv_sem=rsem_r.at[slot], device_id=place(d), device_id_type=MESH,
        )

    def copy_rest(d, slot, count=1):
        return pltpu.make_async_remote_copy(
            src_ref=send_s.at[pl.ds(d, count)], dst_ref=recv_s.at[pl.ds(slot, count)],
            send_sem=send_sem.at[5], recv_sem=rsem_b.at[2], device_id=place(d),
            device_id_type=MESH,
        )

    def copy_x(s, n, count=1):
        return pltpu.make_async_remote_copy(
            src_ref=recv_r.at[pl.ds(s, count)], dst_ref=recv_x.at[pl.ds(s, count)],
            send_sem=send_sem.at[1], recv_sem=rsem_x.at[n],
            device_id=partner, device_id_type=MESH,
        )

    def copy_many(source, target, kind, recv_sem, d, slot, count=1):
        return pltpu.make_async_remote_copy(
            src_ref=source.at[pl.ds(d, count)], dst_ref=target.at[pl.ds(slot, count)],
            send_sem=send_sem.at[kind], recv_sem=recv_sem, device_id=place(d),
            device_id_type=MESH,
        )

    def copy_l(d, slot, n, count=1):
        return copy_many(send_l, recv_l, 2, rsem_l.at[0], d, slot, count)

    def copy_e(d, slot, count=1):
        return copy_many(send_e, recv_e, 3, rsem_b.at[0], d, slot, count)

    def copy_b(d, slot, count=1):
        return copy_many(send_b, recv_b, 4, rsem_b.at[1], d, slot, count)

    for turn in range(2):
        first = (1 - side if turn == 0 else side) * half
        with jax.named_scope(f"gated_r{turn}"):
            value = gated(2 * hidden, first, 0, flat)
            extra = gated(0, first, flat_m, flat)
            for part in range(half_groups):
                at = slice(part * gc, (part + 1) * gc)
                send_r[first // gc + part] = fold(value[at])
                send_s[first // gc + part] = fold(extra[at])
        if turn == 0:
            with jax.named_scope("barrier"):
                pl.semaphore_wait(barrier, groups)
        with jax.named_scope("start_r"):
            if turn == 0:
                order = [(plane, n) for n in range(2) for plane in (far_a, far_b)]
            else:
                order = [(sibling, n) for n in range(along_z)]
                order += [(py, n) for n in range(1, along_z)]
                order += [(plane, n) for n in range(2, along_z) for plane in (far_a, far_b)]
            for plane, n in order:
                copy_r(to(plane, n), me).start()
            if turn == 1:
                for n in range(along_z):
                    for plane in (far_a, far_b, sibling, py):
                        if n == 0 and plane is py:
                            continue
                        copy_rest(to(plane, n), me).start()
    recv_r[me] = send_r[me]
    recv_s[me] = send_s[me]
    copy_x(me, 0).start()

    for turn in range(2):
        first = (1 - side if turn == 0 else side) * half
        with jax.named_scope(f"gated_l{turn}"):
            value = gated(0, first, 0, flat_m)
            for part in range(half_groups):
                send_l[first // gc + part, :, 0:flat_m] = value[
                    part * gc : (part + 1) * gc
                ].astype(jnp.bfloat16)
    recv_l[me] = send_l[me]

    with jax.named_scope("gate"):
        loads[3].wait()
        loads[4].wait()
        gate_f32[...] = 0.5 + 0.5 * jnp.tanh(
            0.5 * jnp.dot(normed_bf[...], gate_ref[...], preferred_element_type=jnp.float32)
        )

    def lift(value, begin, width, lane):
        low, high = begin // LANES, (begin + width - 1) // LANES
        shift = (lane - begin) % LANES

        def turned(n):
            block = value[:, n * LANES : (n + 1) * LANES]
            return block if shift == 0 else pltpu.roll(block, shift, 1)

        if low == high:
            return turned(low)
        return jnp.where(lane8 < lane + high * LANES - begin, turned(low), turned(high))

    def spread_main(value, s, target):
        for k in range(cols):
            at = pl.multiple_of((s * cols + k) * gc, gc)
            target[pl.ds(at, gc), :] = lift(value, k * main, main, 0)

    def spread_right(value, s, target):
        for k in range(cols):
            at = pl.multiple_of((s * cols + k) * gc, gc)
            target[pl.ds(at, gc), :] = jnp.where(
                lane8 < main,
                lift(value, k * main, main, 0),
                lift(value, flat_m + k * edge, edge, main),
            )

    planes = (py, far_a, far_b, sibling)

    def forward(plane, n):
        s = to(plane, n)
        copy_r(s, s).wait_recv()
        copy_x(s, n).start()

    def spread_r(s):
        spread_right(unfold(recv_r[s].astype(jnp.float32), flat), s, right_s.at[px])

    def take_plane(plane, first):
        for n in range(first, along_z):
            forward(plane, n)
        for n in range(along_z):
            spread_r(to(plane, n))

    def take_far(n, carry):
        for plane in (far_a, far_b):
            forward(plane, n)
        for plane in (far_a, far_b):
            spread_r(to(plane, n))
        return carry

    def start_l():
        for plane in (far_a, far_b, sibling, py):
            for n in range(0 if plane is not py else 1, along_z):
                copy_l(to(plane, n), me, n).start()

    with jax.named_scope("take_own"):
        take_plane(py, 1)
    with jax.named_scope("take_far0"):
        take_far(0, 0)
    with jax.named_scope("take_sib"):
        take_plane(sibling, 0)
    with jax.named_scope("take_far1"):
        take_far(1, 0)
    with jax.named_scope("wait_send"):
        pltpu.make_async_remote_copy(
            src_ref=send_r.at[0 : groups - 1], dst_ref=recv_r.at[0 : groups - 1],
            send_sem=send_sem.at[0], recv_sem=rsem_r.at[0], device_id=partner,
            device_id_type=MESH,
        ).wait_send()
    with jax.named_scope("start_l"):
        start_l()
    with jax.named_scope("take_far2"):
        take_far(2, 0)
    with jax.named_scope("take_far3"):
        take_far(3, 0)

    copy_rest(0, 0, groups - 1).wait_recv()

    def take_rest(n, carry):
        for plane in planes:
            s = to(plane, n)
            value = unfold(recv_s[s].astype(jnp.float32), flat_e)
            for k in range(cols):
                at = pl.multiple_of((s * cols + k) * gc, gc)
                edge_s[pl.ds(at, gc), :] = lift(value, k * edge, edge, 0)
        return carry

    with jax.named_scope("take_rest"):
        lax.fori_loop(0, along_z, take_rest, 0, unroll=True)

    def tri(left, width, c, h, first):
        if first:
            right = right_s[h, pl.ds(c, residues, stride=gc), :].T.astype(jnp.bfloat16)
            right_bf[h, c] = right
        else:
            right = right_bf[h, c]
        block = jnp.dot(right[0:rows], left[:, 0:width], preferred_element_type=jnp.float32)
        at = pl.multiple_of(h * rows * gc, gc)
        tri_s[pl.ds(at + c, rows, stride=gc), 0:width] = block

    with jax.named_scope("tri_own"):
        for c in range(gc):
            left = edge_s[pl.ds(c, residues, stride=gc), :].astype(jnp.bfloat16)
            edge_bf[c] = left
            tri(left, edge, c, px, True)

    def take_x(n, carry):
        pltpu.make_async_remote_copy(
            src_ref=recv_r.at[0:along_y], dst_ref=recv_x.at[0:along_y],
            send_sem=send_sem.at[1], recv_sem=rsem_x.at[n], device_id=partner,
            device_id_type=MESH,
        ).wait_recv()
        for plane in planes:
            s = to(plane, n)
            spread_right(unfold(recv_x[s].astype(jnp.float32), flat), s, right_s.at[1 - px])
        return carry

    with jax.named_scope("take_x"):
        lax.fori_loop(0, along_z, take_x, 0)

    def pack(d, width):
        blocks = [None] * (up(cols * width, LANES) // LANES)
        for j in range(cols):
            at = pl.multiple_of((d * cols + j) * gc, gc)
            shift = j * width % LANES
            piece = tri_s[pl.ds(at, gc), :]
            piece = piece if shift == 0 else pltpu.roll(piece, shift, 1)
            n = j * width // LANES
            blocks[n] = piece if shift == 0 else jnp.where(lane8 < shift, blocks[n], piece)
            if shift + width > LANES:
                blocks[n + 1] = piece
        value = jnp.concatenate(blocks, axis=1)
        if width == main:
            return value.astype(jnp.bfloat16)
        return fold(value[:, 0 : cols * width])

    def ship(width, buffer, landed, copy):
        def fill(goals):
            packed = [pack(d, width) for d in goals]
            for d, value in zip(goals, packed):
                buffer[d] = value

        def begin(goals):
            for d in goals:

                @pl.when(d != me)
                def _():
                    copy(d, me).start()

        far = [to(plane, n) for plane in (far_a, far_b) for n in range(along_z)]
        near = [to(plane, n) for plane in (sibling, py) for n in range(along_z)]
        fill(far)
        begin(far)
        fill(near)
        begin(near)
        landed[me] = buffer[me]

    with jax.named_scope("tri_e"):
        for c in range(gc):
            tri(edge_bf[c], edge, c, 1 - px, True)
    with jax.named_scope("ship_e"):
        ship(edge, send_e, recv_e, copy_e)

    with jax.named_scope("take_l"):
        copy_l(0, 0, 0, groups - 1).wait_recv()
        for n in range(along_z):
            for plane in planes:
                s = to(plane, n)
                spread_main(recv_l[s].astype(jnp.float32), s, left_s)
    with jax.named_scope("tri_m"):
        for c in range(gc):
            left = left_s[pl.ds(c, residues, stride=gc), :].astype(jnp.bfloat16)
            for h in range(2):
                tri(left, main, c, h, False)
    with jax.named_scope("ship_m"):
        ship(main, send_b, recv_b, copy_b)

    def final(received, low, width):
        count = width * cols
        if width == main:
            triangle = received[:, :, 0:count].astype(jnp.float32)
        else:
            triangle = jnp.concatenate(
                [unfold(received[s].astype(jnp.float32), count)[:, 0:count] for s in range(groups)],
                axis=0,
            )
        triangle = triangle.reshape(hidden, count)
        normed_tri = layer_norm_lead(triangle).astype(jnp.bfloat16)
        mixed = lax.dot_general(
            normed_tri, out_w_ref[...], (((0,), (0,)), ((), ())),
            preferred_element_type=jnp.float32,
        )
        first = 0 if low == 0 else flat_m
        update = (gate_f32[first : first + count] * mixed).astype(jnp.bfloat16)
        for j in range(cols):
            out_ref[j, low : low + width] = update[j * width : (j + 1) * width]

    with jax.named_scope("take_e"):
        copy_e(0, 0, groups - 1).wait_recv()
    with jax.named_scope("final_e"):
        final(recv_e, main, edge)
    with jax.named_scope("finish"):
        copy_rest(0, 0, groups - 1).wait_send()
        copy_x(0, 0, groups).wait_send()
        copy_l(0, 0, 0, groups - 1).wait_send()
        copy_e(0, 0, groups - 1).wait_send()
    with jax.named_scope("take_b"):
        copy_b(0, 0, groups - 1).wait_recv()
    with jax.named_scope("final_m"):
        final(recv_b, 0, main)
    with jax.named_scope("finish_b"):
        copy_b(0, 0, groups - 1).wait_send()


def scratch_list(main, rows, cols, chans, hidden, groups, residues):
    gc = hidden // groups
    flat_m, flat_e = main * cols, (rows - main) * cols
    flat = flat_m + flat_e
    bf, f32 = jnp.bfloat16, jnp.float32
    return [
        ((cols, rows, chans), bf),
        ((1, residues), jnp.int32),
        ((chans, 4 * hidden), bf),
        ((chans, chans), bf),
        ((hidden, chans), bf),
        ((4 * hidden, chans), bf),
        ((rows * cols, chans), bf),
        ((rows * cols, chans), bf),
        ((rows * cols, chans), f32),
        ((groups, gc // 2, folded(flat)), bf),
        ((groups, gc // 2, folded(flat)), bf),
        ((groups, gc // 2, folded(flat)), bf),
        ((groups, gc // 2, folded(flat_e)), bf),
        ((groups, gc // 2, folded(flat_e)), bf),
        ((groups, gc, up(flat_m, LANES)), bf),
        ((groups, gc, up(flat_m, LANES)), bf),
        ((residues * gc, LANES), f32),
        ((residues * gc, LANES), f32),
        ((gc, residues, LANES), bf),
        ((2, residues * gc, LANES), f32),
        ((2, gc, LANES, residues), bf),
        ((residues * gc, LANES), f32),
        ((groups, gc // 2, folded(flat_e)), bf),
        ((groups, gc // 2, folded(flat_e)), bf),
        ((groups, gc, up(flat_m, LANES)), bf),
        ((groups, gc, up(flat_m, LANES)), bf),
    ]


def fits_kernel(sizes, rows, cols, chans, hidden, residues):
    groups = sizes["gy"] * sizes["gz"]
    main = main_rows(rows)
    edge = rows - main
    if sizes["gx"] != 2 or hidden % (4 * groups) or hidden // groups != 8:
        return False
    if sizes["gy"] != 4 or sizes["gz"] != 4 or residues != 2 * rows or residues != groups * cols:
        return False
    if chans != LANES or rows > LANES or rows % 16 or main < 16 or edge < 16:
        return False
    if rows * cols % LANES * 2 > LANES or edge * cols % LANES * 2 > LANES:
        return False
    total = 0
    for shape, kind in scratch_list(main, rows, cols, chans, hidden, groups, residues):
        count = 1
        for extent in shape:
            count *= extent
        total += count * jnp.dtype(kind).itemsize
    return total < VMEM_BUDGET // 3


def local_fused(sizes, pair_map, residue_mask, proj_weight, gate_weight, out_weight):
    rows, cols, chans = pair_map.shape
    hidden = out_weight.shape[0]
    residues = residue_mask.shape[0]
    if not fits_kernel(sizes, rows, cols, chans, hidden, residues):
        return local(pair_map, residue_mask, proj_weight, gate_weight, out_weight)
    groups = sizes["gy"] * sizes["gz"]
    main = main_rows(rows)
    dma = pltpu.SemaphoreType.DMA
    vmem = pl.BlockSpec(memory_space=pltpu.VMEM)
    turned = pl.pallas_call(
        functools.partial(fused_kernel, sizes["gy"], sizes["gz"], main),
        out_shape=pltpu.VMEM((cols, rows, chans), jnp.bfloat16),
        in_specs=[pl.BlockSpec(memory_space=pltpu.HBM)] * 5,
        out_specs=vmem,
        scratch_shapes=[
            pltpu.VMEM(shape, kind)
            for shape, kind in scratch_list(main, rows, cols, chans, hidden, groups, residues)
        ]
        + [dma((5,)), dma((6,)), dma((groups,)), dma((sizes["gz"],)), dma((1,)), dma((3,))],
        compiler_params=pltpu.CompilerParams(
            collective_id=0, has_side_effects=True, vmem_limit_bytes=VMEM_ALL - 204800
        ),
    )(
        pair_map.transpose(1, 0, 2), residue_mask.reshape(1, residues),
        proj_weight, gate_weight, out_weight,
    )
    return turned.transpose(1, 0, 2)


def solution(mesh):
    placed = (P("gx", ("gy", "gz"), None), P(), P(), P(), P())
    return jax.shard_map(
        functools.partial(local_fused, dict(mesh.shape)), mesh=mesh, in_specs=placed, out_specs=P("gx", ("gy", "gz"), None), check_vma=False
    )
```
